256 devices in a mesh: slab: 64 (over z, x, core), grp: 4 (over y).
Axes of the slice: x: 4, y: 4, z: 8, core: 2. Of those that a mesh axis runs over, the one named last changes fastest.
Arguments:
- iterate: float32 [24576, 256], P(('slab', 'grp')), may hold values from -6 to 6
- residual: float32 [24576, 256], P(('slab', 'grp')), may hold values from -6 to 6
- direction: float32 [24576, 256], P(('slab', 'grp')), may hold values from -6 to 6
- prior_rho: float32 [256], replicated, may hold values from 12288 to 49152
- diag_blocks: float32 [24576, 384], P(('slab', 'grp')), as said below
- lower_coupling: float32 [24576, 128], P(('slab', 'grp')), may hold values from -0.125 to 0.125
- upper_coupling: float32 [24576, 128], P(('slab', 'grp')), may hold values from -0.125 to 0.125
- interface: int32 [64, 128], P('slab'), may hold values from 0 to 383, as said below
- jacobi_inverse: float32 [24576, 96], P(('slab', 'grp'))
- slab_inverse: float32 [24576, 384], P(('slab', 'grp'))
- lower_factor: float32 [24576, 128], P(('slab', 'grp')), may hold values from -0.875 to 0.875
- upper_factor: float32 [24576, 128], P(('slab', 'grp')), may hold values from -0.5 to 0.5
Outputs:
- new_iterate: float32 [24576, 256], P(('slab', 'grp'))
- new_residual: float32 [24576, 256], P(('slab', 'grp'))
- new_direction: float32 [24576, 256], P(('slab', 'grp'))
- new_rho: float32 [256], replicated
The draws below stay inside these ranges and needn't reach their ends.
Inputs may be any that keep to these rules, and one draw needn't show every extreme that they name: `interface`: row k lists 128 distinct dof numbers of slab k. `diag_blocks`: each diagonal block is a positive diagonal plus a skew-symmetric part.
All inputs are finite; a program needn't handle non-finite values.
Results may differ from the reference program's by a relative error of at most 0.0003.
Values sent between devices are 32-bit elements; how exact they have to be, the bound alone decides.
No kernel may reach another device: no remote copies, remote signals or barrier semaphores. Data moves between devices by JAX's collectives and lax.ppermute only.
A program may use at most 64 MiB of HBM per device.

```python
import math
import jax
import jax.numpy as jnp
from jax import lax

B = 384
IF = 128
R = 256
NSLAB = 64
GB = 96
ROWS = 24576
N_GRP = 4


def draw_diag_blocks(key, part):
    first, second = jax.random.split(jax.random.fold_in(key, 11))
    source = jax.random.normal(first, (NSLAB, B, B), jnp.float32) / B ** 0.5
    scales = jax.random.uniform(second, (NSLAB, B), jnp.float32, 1.0, 3.0)
    blocks = source - jnp.swapaxes(source, 1, 2) + scales[:, :, None] * jnp.eye(B, dtype=jnp.float32)[None]
    return blocks.reshape(NSLAB * B, B)


def draw_interface(key, part):
    keys = jax.random.split(jax.random.fold_in(key, 12), NSLAB)
    chosen = jax.vmap(lambda single: jax.random.permutation(single, B)[:IF])(keys)
    return chosen.astype(jnp.int32)


def draw_jacobi_inverse(key, part):
    noise = jax.random.normal(jax.random.fold_in(key, 13), (NSLAB * B, GB), jnp.float32) * (0.5 / GB ** 0.5)
    rowid = jnp.arange(NSLAB * B, dtype=jnp.int32)[:, None] % GB
    colid = jnp.arange(GB, dtype=jnp.int32)[None, :]
    return noise + 0.5 * (rowid == colid).astype(jnp.float32)


def draw_slab_inverse(key, part):
    noise = jax.random.normal(jax.random.fold_in(key, 14), (NSLAB * B, B), jnp.float32) * (0.3 / B ** 0.5)
    rowid = jnp.arange(NSLAB * B, dtype=jnp.int32)[:, None] % B
    colid = jnp.arange(B, dtype=jnp.int32)[None, :]
    return noise + 0.5 * (rowid == colid).astype(jnp.float32)


def steps_of(stream_key, extent, cuts, smallest, high):
    factor_of = 1.0
    for position, parts in cuts:
        draws = jax.random.uniform(jax.random.fold_in(jax.random.fold_in(stream_key, 6), position), (parts,), jnp.float32, smallest / len(cuts), high / len(cuts))
        factor_of = factor_of * jnp.repeat(jnp.exp(draws), extent[position] // parts).reshape((-1,) + (1,) * (len(extent) - 1 - position))
    return factor_of


def gaussian(stream_key, extent, spread, limit, cuts=(), kind=jnp.bfloat16):
    array = spread * jax.random.normal(stream_key, extent, jnp.float32)
    if cuts:
        array = array * steps_of(stream_key, extent, cuts, -0.22, 0.18)
    return jnp.clip(array, -limit, limit).astype(kind)


def setup_inputs(seed: int = 0) -> dict:
    arg_keys = jax.random.split(jax.random.key(seed), 13)
    iterate = gaussian(arg_keys[0], (ROWS, R), 1.0, 6.0, ((0, 256),), jnp.float32)
    residual = gaussian(arg_keys[1], (ROWS, R), 1.0, 6.0, ((0, 256),), jnp.float32)
    direction = gaussian(arg_keys[2], (ROWS, R), 1.0, 6.0, ((0, 256),), jnp.float32)
    prior_rho = jnp.clip(jnp.exp(jax.random.uniform(arg_keys[3], (R,), jnp.float32, math.log(12288.0), math.log(49152.0))), 12288.0, 49152.0)
    diag_blocks = draw_diag_blocks(jax.random.fold_in(arg_keys[12], 71), 0)
    lower_coupling = gaussian(arg_keys[5], (ROWS, IF), (16 * IF) ** -0.5, 0.125, ((0, 256),), jnp.float32)
    upper_coupling = gaussian(arg_keys[6], (ROWS, IF), (16 * IF) ** -0.5, 0.125, ((0, 256),), jnp.float32)
    interface = draw_interface(jax.random.fold_in(arg_keys[12], 71), 0)
    jacobi_inverse = draw_jacobi_inverse(jax.random.fold_in(arg_keys[12], 71), 0)
    slab_inverse = draw_slab_inverse(jax.random.fold_in(arg_keys[12], 71), 0)
    lower_factor = gaussian(arg_keys[10], (ROWS, IF), (IF * 13 // 36) ** -0.5, 0.875, ((0, 256),), jnp.float32)
    upper_factor = gaussian(arg_keys[11], (ROWS, IF), (IF * 17 // 16) ** -0.5, 0.5, ((0, 256),), jnp.float32)
    return {"iterate": iterate, "residual": residual, "direction": direction, "prior_rho": prior_rho, "diag_blocks": diag_blocks, "lower_coupling": lower_coupling, "upper_coupling": upper_coupling, "interface": interface, "jacobi_inverse": jacobi_inverse, "slab_inverse": slab_inverse, "lower_factor": lower_factor, "upper_factor": upper_factor}


def pick_rows(field, interface):
    return jax.vmap(lambda block, index: block[index])(field, interface)


def slab_apply(matrix, field):
    return jnp.einsum("kij,kjr->kir", matrix, field, precision=lax.Precision.HIGHEST)


def operate(field, diag_blocks, lower_coupling, upper_coupling, interface):
    faces = pick_rows(field, interface)
    zero_face = jnp.zeros_like(faces[:1])
    below = jnp.concatenate([zero_face, faces[:-1]], axis=0)
    above = jnp.concatenate([faces[1:], zero_face], axis=0)
    return slab_apply(diag_blocks, field) + slab_apply(lower_coupling, below) + slab_apply(upper_coupling, above)


def affine_step(carry, inputs):
    transfer, offset = inputs
    value = offset + jnp.dot(transfer, carry, precision=lax.Precision.HIGHEST)
    return value, carry


def reference(iterate, residual, direction, prior_rho, diag_blocks, lower_coupling, upper_coupling, interface, jacobi_inverse, slab_inverse, lower_factor, upper_factor):
    shape3 = (NSLAB, B, R)
    iterate_s = iterate.reshape(shape3)
    residual_s = residual.reshape(shape3)
    direction_s = direction.reshape(shape3)
    diag_s = diag_blocks.reshape(NSLAB, B, B)
    lower_s = lower_coupling.reshape(NSLAB, B, IF)
    upper_s = upper_coupling.reshape(NSLAB, B, IF)
    image = operate(direction_s, diag_s, lower_s, upper_s, interface)
    curvature = jnp.sum(direction_s * image, axis=(0, 1))
    step_size = prior_rho / curvature
    new_iterate = iterate_s + step_size * direction_s
    new_residual = residual_s - step_size * image
    jacobi_s = jacobi_inverse.reshape(NSLAB * N_GRP, GB, GB)
    smoothed = slab_apply(jacobi_s, new_residual.reshape(NSLAB * N_GRP, GB, R)).reshape(shape3)
    defect = new_residual - operate(smoothed, diag_s, lower_s, upper_s, interface)
    inverse_s = slab_inverse.reshape(NSLAB, B, B)
    solved = slab_apply(inverse_s, defect)
    factor = slab_apply(inverse_s, lower_factor.reshape(NSLAB, B, IF))
    offsets = pick_rows(solved, interface)
    transfer = -pick_rows(factor, interface)
    upper_f = upper_factor.reshape(NSLAB, B, IF)
    upper_iface = -pick_rows(upper_f, interface)
    start = jnp.zeros((IF, R), jnp.float32)
    _, forward_prev = lax.scan(affine_step, start, (transfer, offsets))
    forward_vals = solved - slab_apply(factor, forward_prev)
    iface_vals = offsets + slab_apply(transfer, forward_prev)
    _, backward_next = lax.scan(affine_step, start, (upper_iface, iface_vals), reverse=True)
    correction = forward_vals - slab_apply(upper_f, backward_next)
    precond = smoothed + correction
    new_rho = jnp.sum(new_residual * precond, axis=(0, 1))
    new_direction = precond + (new_rho / prior_rho) * direction_s
    return (new_iterate.reshape(ROWS, R), new_residual.reshape(ROWS, R), new_direction.reshape(ROWS, R), new_rho)
```

```python
import functools

import jax
import jax.numpy as jnp
from jax import lax
from jax.experimental import pallas as pl
from jax.experimental.pallas import tpu as pltpu
from jax.sharding import Mesh
from jax.sharding import PartitionSpec as P

SLAB = ("slab_0", "slab_1", "slab_2")
PLANE = ("slab_1", "slab_2")
SLAB_GRP = ("slab_0", "slab_1", "slab_2", "grp")
HIGH = lax.Precision.HIGHEST


def mm(left, right, left_dim=1, right_dim=0):
    return lax.dot_general(
        left,
        right,
        (((left_dim,), (right_dim,)), ((), ())),
        precision=HIGH,
        preferred_element_type=jnp.float32,
    )


def to_each(pieces, axes):
    return lax.all_to_all(pieces, axes, split_axis=0, concat_axis=0, tiled=True)


def to_all(x, axes, count):
    return to_each(jnp.broadcast_to(x, (count, *x.shape)), axes)


def beside(faces):
    count = lax.axis_size(SLAB)
    below = lax.ppermute(faces, SLAB, [(i, i + 1) for i in range(count - 1)])
    above = lax.ppermute(faces, SLAB, [(i + 1, i) for i in range(count - 1)])
    return below, above


def swapped(rows):
    half = rows.shape[0] // 2
    return jnp.concatenate([rows[half:], rows[:half]], axis=0)


def in_lanes(first, second, shape):
    lane = lax.broadcasted_iota(jnp.int32, shape, 1)
    return jnp.where(lane == 0, first, jnp.where(lane == 1, second, 0.0))


def sweep_plane(got_ref, states_f_ref, states_b_ref, maps_ref, sums_ref):
    n = got_ref.shape[0]
    width = got_ref.shape[2]
    row = lax.broadcasted_iota(jnp.int32, (width, width), 0)
    lane = lax.broadcasted_iota(jnp.int32, (width, width), 1)
    eye = jnp.where(row == lane, 1.0, 0.0).astype(jnp.float32)
    f = jnp.concatenate([eye, jnp.zeros((16, width), jnp.float32)], axis=0)
    empty = jnp.zeros((width, width), jnp.float32)
    passed = []
    for i in range(n):
        states_f_ref[i] = f
        f = mm(f, got_ref[i, 0:128], 1, 1)
        f = jnp.concatenate([f[:128], f[128:] + got_ref[i, 256:272]], axis=0)
        passed.append(f)
    b = jnp.concatenate([eye, empty, jnp.zeros((16, width), jnp.float32)], axis=0)
    for i in reversed(range(n)):
        states_b_ref[i] = b
        b = mm(b, got_ref[i, 128:256], 1, 1)
        b = jnp.concatenate([b[:128], b[128:] + passed[i]], axis=0)
    maps_ref[0] = f[:128]
    maps_ref[1] = b[:128]
    maps_ref[2] = b[128:256]
    gamma = jnp.zeros((16, width), jnp.float32)
    delta = gamma
    same = gamma
    cross = gamma
    total = jnp.zeros((8, width), jnp.float32)
    for i in range(n):
        g = got_ref[i, 272:288]
        h = got_ref[i, 288:304]
        total = total + got_ref[i, 304:312]
        gamma = gamma + mm(g, states_f_ref[i, 0:128], 1, 1) + mm(h, states_b_ref[i, 128:256], 1, 1)
        delta = delta + mm(h, states_b_ref[i, 0:128], 1, 1)
        own_f = states_f_ref[i, 128:144]
        own_b = states_b_ref[i, 256:272]
        same = same + g * own_f + h * own_b
        cross = cross + g * swapped(own_f) + h * swapped(own_b)
    sums_ref[0:16] = f[128:]
    sums_ref[16:32] = b[256:]
    sums_ref[32:48] = gamma
    sums_ref[48:64] = delta
    sums_ref[64:80] = in_lanes(
        jnp.sum(same, axis=1, keepdims=True), jnp.sum(cross, axis=1, keepdims=True), (16, width)
    )
    sums_ref[80:88] = total


def solve_planes(place_ref, sums_ref, maps_ref, states_f_ref, states_b_ref, out_ref, total_ref, f_ref, b_ref):
    n = sums_ref.shape[0]
    width = sums_ref.shape[2]

    def whole(z, which):
        return jnp.concatenate(
            [maps_ref[p, z, 16 * which : 16 * which + 16] for p in range(maps_ref.shape[0])], axis=0
        )

    f = jnp.zeros((16, width), jnp.float32)
    for z in range(n):
        f_ref[z] = f
        if z + 1 < n:
            f = mm(f, whole(z, 0)) + sums_ref[z, 0:16]
    b = jnp.zeros((16, width), jnp.float32)
    for z in reversed(range(n)):
        b_ref[z] = b
        if z > 0:
            b = mm(b, whole(z, 1)) + (mm(f_ref[z], whole(z, 2)) + sums_ref[z, 16:32])
    same = jnp.zeros((16, width), jnp.float32)
    cross = same
    known = same
    total = jnp.zeros((8, width), jnp.float32)
    for z in range(n):
        gamma = sums_ref[z, 32:48]
        delta = sums_ref[z, 48:64]
        f = f_ref[z]
        b = b_ref[z]
        same = same + gamma * f + delta * b
        cross = cross + gamma * swapped(f) + delta * swapped(b)
        known = known + sums_ref[z, 64:80]
        total = total + sums_ref[z, 80:88]
    dots = known + in_lanes(
        jnp.sum(same, axis=1, keepdims=True), jnp.sum(cross, axis=1, keepdims=True), (16, width)
    )
    total_ref[...] = total
    f = f_ref[place_ref[0]]
    b = b_ref[place_ref[0]]
    for i in range(states_f_ref.shape[0]):
        out_ref[i, 0:16] = mm(f, states_f_ref[i, 0:128]) + states_f_ref[i, 128:144]
        out_ref[i, 16:32] = (
            mm(b, states_b_ref[i, 0:128]) + mm(f, states_b_ref[i, 128:256]) + states_b_ref[i, 256:272]
        )
        out_ref[i, 32:48] = dots


def shaped(*shape):
    return jax.ShapeDtypeStruct(shape, jnp.float32)


VMEM = pl.BlockSpec(memory_space=pltpu.VMEM)
SMEM = pl.BlockSpec(memory_space=pltpu.SMEM)


def plane_kernel(got):
    n, _, width = got.shape
    return pl.pallas_call(
        sweep_plane,
        out_shape=(
            shaped(n, 144, width),
            shaped(n, 272, width),
            shaped(3, 128, width),
            shaped(88, width),
        ),
        in_specs=[VMEM],
        out_specs=(VMEM, VMEM, VMEM, VMEM),
        name="sweep_plane",
    )(got)


def planes_kernel(place, sums, maps, states_f, states_b):
    n = sums.shape[0]
    width = sums.shape[2]
    return pl.pallas_call(
        solve_planes,
        out_shape=(shaped(states_f.shape[0], 48, width), shaped(8, width)),
        in_specs=[SMEM, VMEM, VMEM, VMEM, VMEM],
        out_specs=(VMEM, VMEM),
        scratch_shapes=[pltpu.VMEM((n, 16, width), jnp.float32), pltpu.VMEM((n, 16, width), jnp.float32)],
        name="solve_planes",
    )(place, sums, maps, states_f, states_b)


def sliced(rows):
    two, n, each = 2, 8, rows.shape[0] // 16
    return rows.reshape(two, n, each, -1).transpose(1, 0, 2, 3).reshape(n, two * each, -1)


def joined(pieces):
    n, both, width = pieces.shape
    return pieces.reshape(n, 2, both // 2, width).transpose(1, 0, 2, 3).reshape(n * both, width)


def local(
    iterate,
    residual,
    direction,
    prior_rho,
    diag_blocks,
    lower_coupling,
    upper_coupling,
    interface,
    jacobi_inverse,
    slab_inverse,
    lower_factor,
    upper_factor,
):
    index_rows = interface[0]
    rows, cols = direction.shape
    groups = lax.axis_size("grp")
    part = cols // groups
    fields = to_each(
        jnp.stack(
            [
                jnp.concatenate(
                    [direction[:, q * part : (q + 1) * part], residual[:, q * part : (q + 1) * part]], axis=1
                )
                for q in range(groups)
            ]
        ),
        "grp",
    ).reshape(groups * rows, 2 * part)
    d = fields[:, :part]
    operator = to_all(
        jnp.concatenate([diag_blocks, lower_coupling, upper_coupling], axis=1), "grp", groups
    ).reshape(groups * rows, -1)
    coarse = to_all(
        jnp.concatenate([slab_inverse, lower_factor, upper_factor, jacobi_inverse], axis=1), "grp", groups
    )
    jacobi = coarse[:, :, 640:]
    coarse = coarse.reshape(groups * rows, -1)
    inverse = coarse[:, 0:384]
    lower = coarse[:, 384:512]
    upper = coarse[:, 512:640]

    below, above = beside(d[index_rows])
    w = mm(operator, jnp.concatenate([d, below, above], axis=0))
    x = jnp.concatenate([fields[:, part:], w], axis=1)
    smoothed = lax.dot_general(
        jacobi,
        x.reshape(groups, rows, 2 * part),
        (((2,), (1,)), ((0,), (0,))),
        precision=HIGH,
        preferred_element_type=jnp.float32,
    ).reshape(groups * rows, 2 * part)
    below, above = beside(smoothed[index_rows])
    defect = x - mm(operator, jnp.concatenate([smoothed, below, above], axis=0))
    both = mm(inverse, jnp.concatenate([defect, lower], axis=1))
    solved, factor = both[:, :128], both[:, 128:]
    at_faces = jnp.concatenate([both, upper], axis=1)[index_rows]
    maps = -at_faces[:, 128:]
    pulled = -mm(x, jnp.concatenate([factor, upper], axis=1), 0, 0)
    y = smoothed + solved
    y_swapped = jnp.concatenate([y[:, part:], y[:, :part]], axis=1)
    d_w = jnp.sum(d * w, axis=0)
    known = jnp.stack(
        [jnp.sum(x * y, axis=0), jnp.sum(x * y_swapped, axis=0), jnp.concatenate([d_w, d_w])]
        + [jnp.zeros((2 * part,), jnp.float32)] * 5
    )
    n_plane = lax.axis_size(PLANE)
    n_z = lax.axis_size("slab_0")
    got = to_each(
        jnp.concatenate(
            [
                jnp.broadcast_to(jnp.concatenate([maps[:, :128], maps[:, 128:]], axis=0), (n_plane, 256, 128)),
                sliced(at_faces[:, :128].T),
                sliced(pulled[:, :128]),
                sliced(pulled[:, 128:]),
                jnp.broadcast_to(known, (n_plane, 8, 128)),
            ],
            axis=1,
        ),
        PLANE,
    )
    states_f, states_b, plane_maps, plane_sums = plane_kernel(got)
    own = lax.dynamic_slice_in_dim(plane_maps, 16 * lax.axis_index(PLANE), 16, axis=1).reshape(48, 128)
    sums = to_all(jnp.concatenate([plane_sums, own], axis=0), "slab_0", n_z)
    all_maps = to_all(sums[:, 88:], PLANE, n_plane)
    place = lax.axis_index("slab_0").astype(jnp.int32).reshape(1)
    entering, total = planes_kernel(place, sums, all_maps, states_f, states_b)
    back = to_each(entering, PLANE)
    f = joined(back[:, 0:16])
    b = joined(back[:, 16:32])
    dots = joined(back[:, 32:48]).T
    own_part = lax.dynamic_slice_in_dim(prior_rho, part * lax.axis_index("grp"), part)
    step_size = own_part / total[2, :part]
    same = total[0] + dots[0]
    cross = total[1] + dots[1]
    new_rho = (
        same[:part] - step_size * (cross[:part] + cross[part:]) + step_size * (step_size * same[part:])
    )
    precond = smoothed + mm(inverse, defect - mm(lower, f, 1, 1)) - mm(upper, b, 1, 1)
    result = precond[:, :part] - step_size * precond[:, part:]
    scales = jnp.broadcast_to(jnp.concatenate([step_size, new_rho]), (groups, 8, 2 * part))
    sent = jnp.concatenate(
        [jnp.concatenate([result, w], axis=1).reshape(groups, rows, 2 * part), scales], axis=1
    )
    out = to_each(sent, "grp")
    result = jnp.concatenate([out[q, :rows, :part] for q in range(groups)], axis=1)
    image = jnp.concatenate([out[q, :rows, part:] for q in range(groups)], axis=1)
    step_size = jnp.concatenate([out[q, rows, :part] for q in range(groups)])
    new_rho = jnp.concatenate([out[q, rows, part:] for q in range(groups)])
    new_iterate = iterate + step_size * direction
    new_residual = residual - step_size * image
    new_direction = result + new_rho / prior_rho * direction
    return (new_iterate, new_residual, new_direction, new_rho)


def solution(mesh):
    split = Mesh(
        mesh.devices.reshape(8, 4, 2, mesh.shape["grp"]), ("slab_0", "slab_1", "slab_2", "grp")
    )
    rows = P(SLAB_GRP, None)
    placed = (rows, rows, rows, P(), rows, rows, rows, P(SLAB, None), rows, rows, rows, rows)
    return jax.shard_map(
        local, mesh=split, in_specs=placed, out_specs=(rows, rows, rows, P()), check_vma=False
    )
```

```python
import jax
import jax.numpy as jnp
from jax import lax
from jax.experimental import pallas as pl
from jax.experimental.pallas import tpu as pltpu
from jax.sharding import Mesh
from jax.sharding import PartitionSpec as P

SLAB = ("slab_0", "slab_1", "slab_2")
PLANE = ("slab_1", "slab_2")
SLAB_GRP = ("slab_0", "slab_1", "slab_2", "grp")
HIGH = lax.Precision.HIGHEST
VMEM = pl.BlockSpec(memory_space=pltpu.VMEM)
SMEM = pl.BlockSpec(memory_space=pltpu.SMEM)


def mm(left, right, left_dim=1, right_dim=0):
    return lax.dot_general(
        left,
        right,
        (((left_dim,), (right_dim,)), ((), ())),
        precision=HIGH,
        preferred_element_type=jnp.float32,
    )


def shaped(*shape):
    return jax.ShapeDtypeStruct(shape, jnp.float32)


def call(body, outs, name, smem, *args, scratch=()):
    return pl.pallas_call(
        body,
        out_shape=outs,
        in_specs=[SMEM] * smem + [VMEM] * (len(args) - smem),
        out_specs=jax.tree.map(lambda _: VMEM, outs),
        scratch_shapes=list(scratch),
        name=name,
    )(*args)


def to_each(pieces, axes):
    return lax.all_to_all(pieces, axes, split_axis=0, concat_axis=0, tiled=True)


def ring(x, axis, step):
    count = lax.axis_size(axis)
    return lax.ppermute(x, axis, [(i, (i + step) % count) for i in range(count)])


def beside(faces):
    count = lax.axis_size(SLAB)
    below = lax.ppermute(faces, SLAB, [(i, i + 1) for i in range(count - 1)])
    above = lax.ppermute(faces, SLAB, [(i + 1, i) for i in range(count - 1)])
    return below, above


def swapped(rows):
    half = rows.shape[0] // 2
    return jnp.concatenate([rows[half:], rows[:half]], axis=0)


def flipped(x):
    half = x.shape[1] // 2
    return jnp.concatenate([x[:, half:], x[:, :half]], axis=1)


def pick(index_ref, source_ref, out_ref, start, negate=False):
    for j in range(128):
        row = source_ref[pl.ds(index_ref[0, j], 1), :]
        out_ref[start + j : start + j + 1, :] = -row if negate else row


def pack(direction_ref, residual_ref, inverse_ref, lower_ref, upper_ref, out_ref):
    d = direction_ref[...]
    r = residual_ref[...]
    for q in range(4):
        out_ref[q, :, 0:128] = jnp.concatenate([d[:, 64 * q : 64 * q + 64], r[:, 64 * q : 64 * q + 64]], axis=1)
        out_ref[q, :, 128:512] = inverse_ref[...]
        out_ref[q, :, 512:640] = lower_ref[...]
        out_ref[q, :, 640:768] = upper_ref[...]


def make_maps(index_ref, got_ref, factor_ref, maps_ref, faces_ref, upper_scr, field_scr, face_scr):
    field_scr[...] = got_ref[:, 0:128]
    pick(index_ref, field_scr, face_scr, 0)
    faces_ref[...] = jnp.concatenate([face_scr[0:64, 0:64], face_scr[64:128, 0:64]], axis=1)
    factor_ref[...] = mm(got_ref[:, 128:512], got_ref[:, 512:640])
    upper_scr[...] = got_ref[:, 640:768]
    pick(index_ref, factor_ref, maps_ref, 0, True)
    pick(index_ref, upper_scr, maps_ref, 128, True)


def smooth(index_ref, grp_ref, got_ref, p0, p1, p2, p3, below_ref, above_ref, x_ref, s_ref, faces_ref):
    d = got_ref[:, 0:64]
    below = jnp.concatenate([below_ref[:, 0:64], below_ref[:, 64:128]], axis=0)
    above = jnp.concatenate([above_ref[:, 0:64], above_ref[:, 64:128]], axis=0)
    v = jnp.concatenate([d, below, above], axis=0)
    for step, piece in enumerate((p0, p1, p2, p3)):
        rows = pl.ds(pl.multiple_of(96 * ((grp_ref[0] + 4 - step) % 4), 8), 96)
        w = mm(piece[:, 0:640], v)
        x = jnp.concatenate([got_ref[rows, 64:128], w], axis=1)
        x_ref[rows, :] = x
        s_ref[rows, :] = mm(piece[:, 640:736], x)
    pick(index_ref, s_ref, faces_ref, 0)


def solve_slab(
    index_ref, grp_ref, got_ref, p0, p1, p2, p3, factor_ref, x_ref, s_ref, below_ref, above_ref,
    defect_ref, out_ref, solved_scr, face_scr
):
    v = jnp.concatenate([s_ref[...], below_ref[...], above_ref[...]], axis=0)
    for step, piece in enumerate((p0, p1, p2, p3)):
        rows = pl.ds(pl.multiple_of(96 * ((grp_ref[0] + 4 - step) % 4), 8), 96)
        defect_ref[rows, :] = x_ref[rows, :] - mm(piece[:, 0:640], v)
    x = x_ref[...]
    solved = mm(got_ref[:, 128:512], defect_ref[...])
    solved_scr[...] = solved
    pick(index_ref, solved_scr, face_scr, 0)
    offsets = face_scr[...].T
    turned = x.T
    pulled_f = -mm(turned, factor_ref[...])
    pulled_b = -mm(turned, got_ref[:, 640:768])
    y = s_ref[...] + solved
    d_w = got_ref[:, 0:128] * flipped(x)
    known = jnp.concatenate(
        [
            jnp.sum(x * y, axis=0, keepdims=True),
            jnp.sum(x * flipped(y), axis=0, keepdims=True),
            jnp.sum(d_w, axis=0, keepdims=True),
            jnp.zeros((5, 128), jnp.float32),
        ],
        axis=0,
    )
    for p in range(8):
        for at, part in enumerate((offsets, pulled_f, pulled_b)):
            out_ref[p, 16 * at : 16 * at + 8] = part[8 * p : 8 * p + 8]
            out_ref[p, 16 * at + 8 : 16 * at + 16] = part[64 + 8 * p : 72 + 8 * p]
        out_ref[p, 48:56] = known


def map_plane(
    x_ref, c_ref, m0, m1, m2, m3, n0, n1, n2, n3, maps_ref, states_f_ref, states_b_ref, plane_ref
):
    for step, (mine, other) in enumerate(((m0, n0), (m1, n1), (m2, n2), (m3, n3))):
        at = 2 * ((x_ref[0] + 4 - step) % 4)
        maps_ref[at + c_ref[0]] = mine[...]
        maps_ref[at + 1 - c_ref[0]] = other[...]
    row = lax.broadcasted_iota(jnp.int32, (128, 128), 0)
    lane = lax.broadcasted_iota(jnp.int32, (128, 128), 1)
    eye = jnp.where(row == lane, 1.0, 0.0).astype(jnp.float32)
    states_f_ref[0] = eye
    f = maps_ref[0, 0:128].T
    passed = [f]
    for i in range(1, 8):
        states_f_ref[i] = f
        f = mm(f, maps_ref[i, 0:128], 1, 1)
        passed.append(f)
    empty = jnp.zeros((128, 128), jnp.float32)
    states_b_ref[7] = jnp.concatenate([eye, empty], axis=0)
    b = jnp.concatenate([maps_ref[7, 128:256].T, passed[7]], axis=0)
    for i in reversed(range(7)):
        states_b_ref[i] = b
        b = mm(b, maps_ref[i, 128:256], 1, 1)
        b = jnp.concatenate([b[:128], b[128:] + passed[i]], axis=0)
    plane_ref[0:128] = f
    plane_ref[128:384] = b


def in_lanes(values, place):
    row = lax.broadcasted_iota(jnp.int32, (16, 128), 0)
    lane = lax.broadcasted_iota(jnp.int32, (16, 128), 1)
    target = jnp.where(row < 8, row + 8 * place, row + 56 + 8 * place)
    return jnp.sum(jnp.where(lane == target, values, 0.0), axis=0, keepdims=True)


def sweep_plane(place_ref, got_ref, maps_ref, states_f_ref, states_b_ref, own_f_ref, own_b_ref, out_ref):
    f = jnp.zeros((16, 128), jnp.float32)
    for i in range(8):
        own_f_ref[i] = f
        into = got_ref[i, 0:16]
        f = into if i == 0 else mm(own_f_ref[i], maps_ref[i, 0:128], 1, 1) + into
    last = f
    b = jnp.zeros((16, 128), jnp.float32)
    for i in reversed(range(8)):
        own_b_ref[i] = b
        b = last if i == 7 else mm(own_b_ref[i], maps_ref[i, 128:256], 1, 1) + own_f_ref[i + 1]
    gamma = jnp.zeros((16, 128), jnp.float32)
    delta = gamma
    same = gamma
    cross = gamma
    total = jnp.zeros((8, 128), jnp.float32)
    for i in range(8):
        g = got_ref[i, 16:32]
        h = got_ref[i, 32:48]
        total = total + got_ref[i, 48:56]
        gamma = gamma + mm(g, states_f_ref[i], 1, 1) + mm(h, states_b_ref[i, 128:256], 1, 1)
        delta = delta + mm(h, states_b_ref[i, 0:128], 1, 1)
        own_f = own_f_ref[i]
        own_b = own_b_ref[i]
        same = same + g * own_f + h * own_b
        cross = cross + g * swapped(own_f) + h * swapped(own_b)
    place = place_ref[0]
    known = jnp.concatenate(
        [
            total[0:3],
            in_lanes(jnp.sum(same, axis=1, keepdims=True), place),
            in_lanes(jnp.sum(cross, axis=1, keepdims=True), place),
            jnp.zeros((3, 128), jnp.float32),
        ],
        axis=0,
    )
    for z in range(8):
        out_ref[z, 0:16] = last
        out_ref[z, 16:32] = b
        out_ref[z, 32:48] = gamma
        out_ref[z, 48:64] = delta
        out_ref[z, 64:72] = known


def solve_planes(
    z_ref, place_ref, sums_ref, a0, a1, a2, a3, a4, b1, b2, b3,
    states_f_ref, states_b_ref, own_f_ref, own_b_ref, out_ref, total_ref, maps_scr, f_scr, b_scr
):
    for step, piece in ((0, a0), (1, a1), (2, a2), (3, a3), (4, a4), (-1, b1), (-2, b2), (-3, b3)):
        maps_scr[(z_ref[0] + 8 - step) % 8] = piece[...]
    f = jnp.zeros((16, 128), jnp.float32)
    for z in range(8):
        f_scr[z] = f
        if z == 0:
            f = sums_ref[z, 0:16]
        elif z < 7:
            f = mm(f, maps_scr[z, 0:128]) + sums_ref[z, 0:16]
    b = jnp.zeros((16, 128), jnp.float32)
    for z in reversed(range(8)):
        b_scr[z] = b
        if z > 0:
            into = mm(f_scr[z], maps_scr[z, 256:384]) + sums_ref[z, 16:32]
            b = into if z == 7 else mm(b, maps_scr[z, 128:256]) + into
    same = jnp.zeros((16, 128), jnp.float32)
    cross = same
    known = jnp.zeros((8, 128), jnp.float32)
    for z in range(8):
        gamma = sums_ref[z, 32:48]
        delta = sums_ref[z, 48:64]
        same = same + gamma * f_scr[z] + delta * b_scr[z]
        cross = cross + gamma * swapped(f_scr[z]) + delta * swapped(b_scr[z])
        known = known + sums_ref[z, 64:72]
    total_ref[...] = known
    place = place_ref[0]
    dots = jnp.concatenate(
        [
            known[3:4] + in_lanes(jnp.sum(same, axis=1, keepdims=True), place),
            known[4:5] + in_lanes(jnp.sum(cross, axis=1, keepdims=True), place),
            jnp.zeros((6, 128), jnp.float32),
        ],
        axis=0,
    )
    f = f_scr[z_ref[0]]
    b = b_scr[z_ref[0]]
    for i in range(8):
        out_ref[i, 0:16] = mm(f, states_f_ref[i]) + own_f_ref[i]
        out_ref[i, 16:32] = mm(b, states_b_ref[i, 0:128]) + mm(f, states_b_ref[i, 128:256]) + own_b_ref[i]
        out_ref[i, 32:40] = dots


def finish(got_ref, back_ref, total_ref, rho_ref, defect_ref, x_ref, s_ref, out_ref):
    def rows(start):
        return jnp.concatenate(
            [back_ref[p, start : start + 8] for p in range(8)]
            + [back_ref[p, start + 8 : start + 16] for p in range(8)],
            axis=0,
        )

    dots = back_ref[0, 32:40]
    for p in range(1, 8):
        dots = dots + back_ref[p, 32:40]
    rest = defect_ref[...] - mm(got_ref[:, 512:640], rows(0), 1, 1)
    precond = s_ref[...] + mm(got_ref[:, 128:512], rest) - mm(got_ref[:, 640:768], rows(16), 1, 1)
    total = total_ref[...]
    step = rho_ref[...] / total[2:3, 0:64]
    same = total[0:1] + dots[0:1]
    cross = total[1:2] + dots[1:2]
    rho = same[:, 0:64] - step * (cross[:, 0:64] + cross[:, 64:128]) + step * (step * same[:, 64:128])
    result = precond[:, 0:64] - step * precond[:, 64:128]
    both = jnp.concatenate([result, x_ref[:, 64:128]], axis=1)
    scales = jnp.broadcast_to(jnp.concatenate([step, rho], axis=1), (8, 128))
    for q in range(4):
        out_ref[q, 0:96] = both[96 * q : 96 * q + 96]
        out_ref[q, 96:104] = scales


def local(
    iterate,
    residual,
    direction,
    prior_rho,
    diag_blocks,
    lower_coupling,
    upper_coupling,
    interface,
    jacobi_inverse,
    slab_inverse,
    lower_factor,
    upper_factor,
):
    def here(axes):
        return lax.axis_index(axes).astype(jnp.int32).reshape(1)

    grp = here("grp")
    part = 64
    operator = jnp.concatenate([diag_blocks, lower_coupling, upper_coupling, jacobi_inverse], axis=1)
    got = to_each(
        call(pack, shaped(4, 96, 768), "pack", 0, direction, residual, slab_inverse, lower_factor, upper_factor),
        "grp",
    ).reshape(384, 768)
    pieces = [operator] + [ring(operator, "grp", step) for step in (1, 2, 3)]
    factor, maps, faces = call(
        make_maps,
        (shaped(384, 128), shaped(256, 128), shaped(64, 128)),
        "make_maps",
        1,
        interface,
        got,
        scratch=[
            pltpu.VMEM((384, 128), jnp.float32),
            pltpu.VMEM((384, 128), jnp.float32),
            pltpu.VMEM((128, 128), jnp.float32),
        ],
    )
    along = [maps] + [ring(maps, "slab_1", step) for step in (1, 2, 3)]
    across = [ring(m, "slab_2", 1) for m in along]
    below, above = beside(faces)
    x, s, faces = call(
        smooth,
        (shaped(384, 128), shaped(384, 128), shaped(128, 128)),
        "smooth",
        2,
        interface,
        grp,
        got,
        *pieces,
        below,
        above,
    )
    below, above = beside(faces)
    defect, sent = call(
        solve_slab,
        (shaped(384, 128), shaped(8, 56, 128)),
        "solve_slab",
        2,
        interface,
        grp,
        got,
        *pieces,
        factor,
        x,
        s,
        below,
        above,
        scratch=[pltpu.VMEM((384, 128), jnp.float32), pltpu.VMEM((128, 128), jnp.float32)],
    )
    maps, states_f, states_b, plane = call(
        map_plane,
        (shaped(8, 256, 128), shaped(8, 128, 128), shaped(8, 256, 128), shaped(384, 128)),
        "map_plane",
        2,
        here("slab_1"),
        here("slab_2"),
        *along,
        *across,
    )
    ups = [plane]
    for _ in range(4):
        ups.append(ring(ups[-1], "slab_0", 1))
    downs = [plane]
    for _ in range(3):
        downs.append(ring(downs[-1], "slab_0", -1))
    place = here(PLANE)
    own_f, own_b, sums = call(
        sweep_plane,
        (shaped(8, 16, 128), shaped(8, 16, 128), shaped(8, 72, 128)),
        "sweep_plane",
        1,
        place,
        to_each(sent, PLANE),
        maps,
        states_f,
        states_b,
    )
    entering, total = call(
        solve_planes,
        (shaped(8, 40, 128), shaped(8, 128)),
        "solve_planes",
        2,
        here("slab_0"),
        place,
        to_each(sums, "slab_0"),
        *ups,
        *downs[1:],
        states_f,
        states_b,
        own_f,
        own_b,
        scratch=[
            pltpu.VMEM((8, 384, 128), jnp.float32),
            pltpu.VMEM((8, 16, 128), jnp.float32),
            pltpu.VMEM((8, 16, 128), jnp.float32),
        ],
    )
    own_rho = lax.dynamic_slice_in_dim(prior_rho, part * grp[0], part).reshape(1, part)
    out = to_each(
        call(
            finish,
            shaped(4, 104, 128),
            "finish",
            0,
            got,
            to_each(entering, PLANE),
            total,
            own_rho,
            defect,
            x,
            s,
        ),
        "grp",
    )
    result = jnp.concatenate([out[q, :96, :part] for q in range(4)], axis=1)
    image = jnp.concatenate([out[q, :96, part:] for q in range(4)], axis=1)
    step_size = jnp.concatenate([out[q, 96, :part] for q in range(4)])
    new_rho = jnp.concatenate([out[q, 96, part:] for q in range(4)])
    new_iterate = iterate + step_size * direction
    new_residual = residual - step_size * image
    new_direction = result + new_rho / prior_rho * direction
    return (new_iterate, new_residual, new_direction, new_rho)


def solution(mesh):
    split = Mesh(
        mesh.devices.reshape(8, 4, 2, mesh.shape["grp"]), ("slab_0", "slab_1", "slab_2", "grp")
    )
    rows = P(SLAB_GRP, None)
    placed = (rows, rows, rows, P(), rows, rows, rows, P(SLAB, None), rows, rows, rows, rows)
    return jax.shard_map(
        local, mesh=split, in_specs=placed, out_specs=(rows, rows, rows, P()), check_vma=False
    )
```

```python
import jax
import jax.numpy as jnp
from jax import lax
from jax.experimental import pallas as pl
from jax.experimental.pallas import tpu as pltpu
from jax.sharding import Mesh
from jax.sharding import PartitionSpec as P

SLAB = ("slab_0", "slab_1", "slab_2")
PLANE = ("slab_1", "slab_2")
SLAB_GRP = ("slab_0", "slab_1", "slab_2", "grp")
VMEM = pl.BlockSpec(memory_space=pltpu.VMEM)
SMEM = pl.BlockSpec(memory_space=pltpu.SMEM)


def halves(x):
    high = x.astype(jnp.bfloat16)
    return high, (x - high.astype(jnp.float32)).astype(jnp.bfloat16)


def mm(left, right, right_dim=0):
    high, low = halves(left)
    right_high, right_low = right if isinstance(right, tuple) else halves(right)

    def dot(a, b):
        return lax.dot_general(
            a, b, (((1,), (right_dim,)), ((), ())), preferred_element_type=jnp.float32
        )

    n = left.shape[0]
    both = dot(jnp.concatenate([high, low], axis=0), right_high)
    return both[:n] + (both[n:] + dot(high, right_low))


def keep(ref, at, x):
    high, low = halves(x)
    ref[0, at] = high
    ref[1, at] = low


def kept(ref, at, rows=slice(None)):
    return ref[0, at, rows], ref[1, at, rows]


def shaped(*shape, dtype=jnp.float32):
    return jax.ShapeDtypeStruct(shape, dtype)


def call(body, outs, smem, *args, scratch=()):
    return pl.pallas_call(
        body,
        out_shape=outs,
        in_specs=[SMEM] * smem + [VMEM] * (len(args) - smem),
        out_specs=jax.tree.map(lambda _: VMEM, outs),
        scratch_shapes=list(scratch),
        compiler_params=pltpu.CompilerParams(vmem_limit_bytes=16 * 1024 * 1024),
    )(*args)


def to_each(pieces, axes):
    return lax.all_to_all(pieces, axes, split_axis=0, concat_axis=0, tiled=True)


def ring(x, axis, step):
    count = lax.axis_size(axis)
    return lax.ppermute(x, axis, [(i, (i + step) % count) for i in range(count)])


def beside(faces):
    count = lax.axis_size(SLAB)
    below = lax.ppermute(faces, SLAB, [(i, i + 1) for i in range(count - 1)])
    above = lax.ppermute(faces, SLAB, [(i + 1, i) for i in range(count - 1)])
    return below, above


def swapped(rows):
    half = rows.shape[0] // 2
    return jnp.concatenate([rows[half:], rows[:half]], axis=0)


def flipped(x):
    half = x.shape[1] // 2
    return jnp.concatenate([x[:, half:], x[:, :half]], axis=1)


def pick(index_ref, source_ref, out_ref):
    for j in range(128):
        out_ref[j : j + 1, :] = source_ref[pl.ds(index_ref[0, j], 1), :]


def pack(direction_ref, residual_ref, inverse_ref, lower_ref, upper_ref, out_ref):
    d = direction_ref[...]
    r = residual_ref[...]
    for q in range(4):
        out_ref[q, :, 0:128] = jnp.concatenate([d[:, 64 * q : 64 * q + 64], r[:, 64 * q : 64 * q + 64]], axis=1)
        out_ref[q, :, 128:512] = inverse_ref[...]
        out_ref[q, :, 512:640] = lower_ref[...]
        out_ref[q, :, 640:768] = upper_ref[...]


def make_maps(index_ref, got_ref, factor_ref, maps_ref, faces_ref, all_scr, face_scr):
    factor = mm(got_ref[:, 128:512], got_ref[:, 512:640])
    factor_ref[...] = factor
    all_scr[:, 0:128] = got_ref[:, 0:128]
    all_scr[:, 128:256] = factor
    all_scr[:, 256:384] = got_ref[:, 640:768]
    pick(index_ref, all_scr, face_scr)
    faces_ref[...] = jnp.concatenate([face_scr[0:64, 0:64], face_scr[64:128, 0:64]], axis=1)
    maps_ref[0:128] = -face_scr[:, 128:256]
    maps_ref[128:256] = -face_scr[:, 256:384]


def smooth(index_ref, grp_ref, got_ref, p0, p1, p2, p3, below_ref, above_ref, x_ref, s_ref, faces_ref):
    below = jnp.concatenate([below_ref[:, 0:64], below_ref[:, 64:128]], axis=0)
    above = jnp.concatenate([above_ref[:, 0:64], above_ref[:, 64:128]], axis=0)
    v = jnp.concatenate([got_ref[:, 0:64], below, above], axis=0)
    pieces = (p0, p1, p2, p3)
    image = mm(jnp.concatenate([piece[:, 0:640] for piece in pieces], axis=0), v)
    for step, piece in enumerate(pieces):
        rows = pl.ds(pl.multiple_of(96 * ((grp_ref[0] + 4 - step) % 4), 8), 96)
        x = jnp.concatenate([got_ref[rows, 64:128], image[96 * step : 96 * step + 96]], axis=1)
        x_ref[rows, :] = x
        s_ref[rows, :] = mm(piece[:, 640:736], x)
    pick(index_ref, s_ref, faces_ref)


def solve_slab(
    index_ref, grp_ref, got_ref, p0, p1, p2, p3, factor_ref, x_ref, s_ref, below_ref, above_ref,
    defect_ref, out_ref, solved_scr, face_scr
):
    v = jnp.concatenate([s_ref[...], below_ref[...], above_ref[...]], axis=0)
    pieces = (p0, p1, p2, p3)
    applied = mm(jnp.concatenate([piece[:, 0:640] for piece in pieces], axis=0), v)
    for step in range(4):
        rows = pl.ds(pl.multiple_of(96 * ((grp_ref[0] + 4 - step) % 4), 8), 96)
        defect_ref[rows, :] = x_ref[rows, :] - applied[96 * step : 96 * step + 96]
    x = x_ref[...]
    solved = mm(got_ref[:, 128:512], defect_ref[...])
    solved_scr[...] = solved
    pick(index_ref, solved_scr, face_scr)
    offsets = face_scr[...].T
    turned = x.T
    pulled = -mm(turned, jnp.concatenate([factor_ref[...], got_ref[:, 640:768]], axis=1))
    y = s_ref[...] + solved
    known = jnp.concatenate(
        [
            jnp.sum(x * y, axis=0, keepdims=True),
            jnp.sum(x * flipped(y), axis=0, keepdims=True),
            jnp.sum(got_ref[:, 0:128] * flipped(x), axis=0, keepdims=True),
            jnp.zeros((5, 128), jnp.float32),
        ],
        axis=0,
    )
    for p in range(8):
        for at, part in enumerate((offsets, pulled[:, 0:128], pulled[:, 128:256])):
            out_ref[p, 16 * at : 16 * at + 8] = part[8 * p : 8 * p + 8]
            out_ref[p, 16 * at + 8 : 16 * at + 16] = part[64 + 8 * p : 72 + 8 * p]
        out_ref[p, 48:56] = known


def map_plane(
    x_ref, c_ref, m0, m1, m2, m3, n0, n1, n2, n3, maps_ref, states_f_ref, states_b_ref, plane_ref,
    all_scr, f_scr
):
    for step, (mine, other) in enumerate(((m0, n0), (m1, n1), (m2, n2), (m3, n3))):
        at = 2 * ((x_ref[0] + 4 - step) % 4)
        all_scr[at + c_ref[0]] = mine[...]
        all_scr[at + 1 - c_ref[0]] = other[...]
    for i in range(8):
        keep(maps_ref, i, all_scr[i])
    row = lax.broadcasted_iota(jnp.int32, (128, 128), 0)
    lane = lax.broadcasted_iota(jnp.int32, (128, 128), 1)
    eye = jnp.where(row == lane, 1.0, 0.0).astype(jnp.float32)
    keep(states_f_ref, 0, eye)
    f_scr[0] = all_scr[0, 0:128].T
    for i in range(1, 8):
        keep(states_f_ref, i, f_scr[i - 1])
        f_scr[i] = mm(f_scr[i - 1], kept(maps_ref, i, slice(0, 128)), 1)
    plane_ref[0:128] = f_scr[7]
    keep(states_b_ref, 7, jnp.concatenate([eye, jnp.zeros((128, 128), jnp.float32)], axis=0))
    plane_ref[128:256] = all_scr[7, 128:256].T
    plane_ref[256:384] = f_scr[7]
    for i in reversed(range(7)):
        keep(states_b_ref, i, plane_ref[128:384])
        b = mm(plane_ref[128:384], kept(maps_ref, i, slice(128, 256)), 1)
        plane_ref[128:256] = b[0:128]
        plane_ref[256:384] = b[128:256] + f_scr[i]


def in_lanes(values, place):
    row = lax.broadcasted_iota(jnp.int32, (16, 128), 0)
    lane = lax.broadcasted_iota(jnp.int32, (16, 128), 1)
    target = jnp.where(row < 8, row + 8 * place, row + 56 + 8 * place)
    return jnp.sum(jnp.where(lane == target, values, 0.0), axis=0, keepdims=True)


def sweep_plane(place_ref, got_ref, maps_ref, states_f_ref, states_b_ref, own_f_ref, own_b_ref, out_ref):
    own_f_ref[0] = jnp.zeros((16, 128), jnp.float32)
    own_f_ref[1] = got_ref[0, 0:16]
    for i in range(1, 8):
        f = mm(own_f_ref[i], kept(maps_ref, i, slice(0, 128)), 1) + got_ref[i, 0:16]
        own_f_ref[i + 1] = f
    own_b_ref[7] = jnp.zeros((16, 128), jnp.float32)
    own_b_ref[6] = own_f_ref[8]
    for i in reversed(range(7)):
        b = mm(own_b_ref[i], kept(maps_ref, i, slice(128, 256)), 1) + own_f_ref[i + 1]
        if i > 0:
            own_b_ref[i - 1] = b
    gamma = jnp.zeros((16, 128), jnp.float32)
    delta = gamma
    same = gamma
    cross = gamma
    total = jnp.zeros((8, 128), jnp.float32)
    for i in range(8):
        g = got_ref[i, 16:32]
        h = got_ref[i, 32:48]
        total = total + got_ref[i, 48:56]
        gamma = gamma + mm(g, kept(states_f_ref, i), 1) + mm(h, kept(states_b_ref, i, slice(128, 256)), 1)
        delta = delta + mm(h, kept(states_b_ref, i, slice(0, 128)), 1)
        own_f = own_f_ref[i]
        own_b = own_b_ref[i]
        same = same + g * own_f + h * own_b
        cross = cross + g * swapped(own_f) + h * swapped(own_b)
    place = place_ref[0]
    known = jnp.concatenate(
        [
            total[0:3],
            in_lanes(jnp.sum(same, axis=1, keepdims=True), place),
            in_lanes(jnp.sum(cross, axis=1, keepdims=True), place),
            jnp.zeros((3, 128), jnp.float32),
        ],
        axis=0,
    )
    for z in range(8):
        out_ref[z, 0:16] = own_f_ref[8]
        out_ref[z, 16:32] = b
        out_ref[z, 32:48] = gamma
        out_ref[z, 48:64] = delta
        out_ref[z, 64:72] = known


def solve_planes(
    z_ref, place_ref, sums_ref, a0, a1, a2, a3, a4, b1, b2, b3,
    states_f_ref, states_b_ref, own_f_ref, own_b_ref, out_ref, total_ref, maps_scr, f_scr, b_scr
):
    for step, piece in ((0, a0), (1, a1), (2, a2), (3, a3), (4, a4), (-1, b1), (-2, b2), (-3, b3)):
        maps_scr[(z_ref[0] + 8 - step) % 8] = piece[...]
    f_scr[0] = jnp.zeros((16, 128), jnp.float32)
    f_scr[1] = sums_ref[0, 0:16]
    for z in range(1, 7):
        f_scr[z + 1] = mm(f_scr[z], maps_scr[z, 0:128]) + sums_ref[z, 0:16]
    b_scr[7] = jnp.zeros((16, 128), jnp.float32)
    for z in range(1, 8):
        b_scr[z - 1] = mm(f_scr[z], maps_scr[z, 256:384]) + sums_ref[z, 16:32]
    for z in reversed(range(1, 7)):
        b_scr[z - 1] = b_scr[z - 1] + mm(b_scr[z], maps_scr[z, 128:256])
    same = jnp.zeros((16, 128), jnp.float32)
    cross = same
    known = jnp.zeros((8, 128), jnp.float32)
    for z in range(8):
        gamma = sums_ref[z, 32:48]
        delta = sums_ref[z, 48:64]
        same = same + gamma * f_scr[z] + delta * b_scr[z]
        cross = cross + gamma * swapped(f_scr[z]) + delta * swapped(b_scr[z])
        known = known + sums_ref[z, 64:72]
    total_ref[...] = known
    place = place_ref[0]
    dots = jnp.concatenate(
        [
            known[3:4] + in_lanes(jnp.sum(same, axis=1, keepdims=True), place),
            known[4:5] + in_lanes(jnp.sum(cross, axis=1, keepdims=True), place),
            jnp.zeros((6, 128), jnp.float32),
        ],
        axis=0,
    )
    f = f_scr[z_ref[0]]
    b = b_scr[z_ref[0]]
    for i in range(8):
        out_ref[i, 0:16] = mm(f, kept(states_f_ref, i)) + own_f_ref[i]
        out_ref[i, 16:32] = (
            mm(b, kept(states_b_ref, i, slice(0, 128)))
            + mm(f, kept(states_b_ref, i, slice(128, 256)))
            + own_b_ref[i]
        )
        out_ref[i, 32:40] = dots


def finish(got_ref, back_ref, total_ref, rho_ref, defect_ref, x_ref, s_ref, out_ref):
    def rows(start):
        return jnp.concatenate(
            [back_ref[p, start : start + 8] for p in range(8)]
            + [back_ref[p, start + 8 : start + 16] for p in range(8)],
            axis=0,
        )

    dots = back_ref[0, 32:40]
    for p in range(1, 8):
        dots = dots + back_ref[p, 32:40]
    rest = defect_ref[...] - mm(got_ref[:, 512:640], rows(0), 1)
    precond = s_ref[...] + mm(got_ref[:, 128:512], rest) - mm(got_ref[:, 640:768], rows(16), 1)
    total = total_ref[...]
    step = rho_ref[...] / total[2:3, 0:64]
    same = total[0:1] + dots[0:1]
    cross = total[1:2] + dots[1:2]
    rho = same[:, 0:64] - step * (cross[:, 0:64] + cross[:, 64:128]) + step * (step * same[:, 64:128])
    result = precond[:, 0:64] - step * precond[:, 64:128]
    both = jnp.concatenate([result, x_ref[:, 64:128]], axis=1)
    scales = jnp.broadcast_to(jnp.concatenate([step, rho], axis=1), (8, 128))
    for q in range(4):
        out_ref[q, 0:96] = both[96 * q : 96 * q + 96]
        out_ref[q, 96:104] = scales


def body(
    iterate,
    residual,
    direction,
    prior_rho,
    diag_blocks,
    lower_coupling,
    upper_coupling,
    interface,
    jacobi_inverse,
    slab_inverse,
    lower_factor,
    upper_factor,
):
    def here(axes):
        return lax.axis_index(axes).astype(jnp.int32).reshape(1)

    grp = here("grp")
    part = 64
    operator = jnp.concatenate([diag_blocks, lower_coupling, upper_coupling, jacobi_inverse], axis=1)
    got = to_each(
        call(pack, shaped(4, 96, 768), 0, direction, residual, slab_inverse, lower_factor, upper_factor),
        "grp",
    ).reshape(384, 768)
    pieces = [operator] + [ring(operator, "grp", step) for step in (1, 2, 3)]
    factor, maps, faces = call(
        make_maps,
        (shaped(384, 128), shaped(256, 128), shaped(64, 128)),
        1,
        interface,
        got,
        scratch=[pltpu.VMEM((384, 384), jnp.float32), pltpu.VMEM((128, 384), jnp.float32)],
    )
    along = [maps] + [ring(maps, "slab_1", step) for step in (1, 2, 3)]
    across = [ring(m, "slab_2", 1) for m in along]
    below, above = beside(faces)
    x, s, faces = call(
        smooth,
        (shaped(384, 128), shaped(384, 128), shaped(128, 128)),
        2,
        interface,
        grp,
        got,
        *pieces,
        below,
        above,
    )
    below, above = beside(faces)
    defect, sent = call(
        solve_slab,
        (shaped(384, 128), shaped(8, 56, 128)),
        2,
        interface,
        grp,
        got,
        *pieces,
        factor,
        x,
        s,
        below,
        above,
        scratch=[pltpu.VMEM((384, 128), jnp.float32), pltpu.VMEM((128, 128), jnp.float32)],
    )
    maps, states_f, states_b, plane = call(
        map_plane,
        (
            shaped(2, 8, 256, 128, dtype=jnp.bfloat16),
            shaped(2, 8, 128, 128, dtype=jnp.bfloat16),
            shaped(2, 8, 256, 128, dtype=jnp.bfloat16),
            shaped(384, 128),
        ),
        2,
        here("slab_1"),
        here("slab_2"),
        *along,
        *across,
        scratch=[pltpu.VMEM((8, 256, 128), jnp.float32), pltpu.VMEM((8, 128, 128), jnp.float32)],
    )
    ups = [plane]
    for _ in range(1, 5):
        ups.append(ring(ups[-1], "slab_0", 1))
    downs = [plane]
    for _ in range(1, 4):
        downs.append(ring(downs[-1], "slab_0", -1))
    place = here(PLANE)
    own_f, own_b, sums = call(
        sweep_plane,
        (shaped(9, 16, 128), shaped(8, 16, 128), shaped(8, 72, 128)),
        1,
        place,
        to_each(sent, PLANE),
        maps,
        states_f,
        states_b,
    )
    entering, total = call(
        solve_planes,
        (shaped(8, 40, 128), shaped(8, 128)),
        2,
        here("slab_0"),
        place,
        to_each(sums, "slab_0"),
        *ups,
        *downs[1:],
        states_f,
        states_b,
        own_f,
        own_b,
        scratch=[
            pltpu.VMEM((8, 384, 128), jnp.float32),
            pltpu.VMEM((8, 16, 128), jnp.float32),
            pltpu.VMEM((8, 16, 128), jnp.float32),
        ],
    )
    own_rho = lax.dynamic_slice_in_dim(prior_rho, part * grp[0], part).reshape(1, part)
    out = to_each(
        call(
            finish,
            shaped(4, 104, 128),
            0,
            got,
            to_each(entering, PLANE),
            total,
            own_rho,
            defect,
            x,
            s,
        ),
        "grp",
    )
    result = jnp.concatenate([out[q, :96, :part] for q in range(4)], axis=1)
    image = jnp.concatenate([out[q, :96, part:] for q in range(4)], axis=1)
    step_size = jnp.concatenate([out[q, 96, :part] for q in range(4)])
    new_rho = jnp.concatenate([out[q, 96, part:] for q in range(4)])
    new_iterate = iterate + step_size * direction
    new_residual = residual - step_size * image
    new_direction = result + new_rho / prior_rho * direction
    return (new_iterate, new_residual, new_direction, new_rho)


def solution(mesh):
    split = Mesh(
        mesh.devices.reshape(8, 4, 2, mesh.shape["grp"]), ("slab_0", "slab_1", "slab_2", "grp")
    )
    rows = P(SLAB_GRP, None)
    placed = (rows, rows, rows, P(), rows, rows, rows, P(SLAB, None), rows, rows, rows, rows)
    return jax.shard_map(
        body, mesh=split, in_specs=placed, out_specs=(rows, rows, rows, P()), check_vma=False
    )
```

```python
import jax
import jax.numpy as jnp
from jax import lax
from jax.experimental import pallas as pl
from jax.experimental.pallas import tpu as pltpu
from jax.sharding import Mesh
from jax.sharding import PartitionSpec as P

SLAB = ("slab_0", "slab_1", "slab_2")
PLANE = ("slab_1", "slab_2")
SLAB_GRP = ("slab_0", "slab_1", "slab_2", "grp")
VMEM = pl.BlockSpec(memory_space=pltpu.VMEM)
SMEM = pl.BlockSpec(memory_space=pltpu.SMEM)


def halves(x):
    high = x.astype(jnp.bfloat16)
    return high, (x - high.astype(jnp.float32)).astype(jnp.bfloat16)


def mm(left, right, right_dim=0):
    high, low = halves(left)
    right_high, right_low = right if isinstance(right, tuple) else halves(right)

    def dot(a, b):
        return lax.dot_general(
            a, b, (((1,), (right_dim,)), ((), ())), preferred_element_type=jnp.float32
        )

    n = left.shape[0]
    both = dot(jnp.concatenate([high, low], axis=0), right_high)
    return both[:n] + (both[n:] + dot(high, right_low))


def keep(ref, at, x):
    high, low = halves(x)
    ref[0, at] = high
    ref[1, at] = low


def kept(ref, at, rows=slice(None)):
    return ref[0, at, rows], ref[1, at, rows]


def shaped(*shape, dtype=jnp.float32):
    return jax.ShapeDtypeStruct(shape, dtype)


def call(body, outs, smem, *args, scratch=()):
    return pl.pallas_call(
        body,
        out_shape=outs,
        in_specs=[SMEM] * smem + [VMEM] * (len(args) - smem),
        out_specs=jax.tree.map(lambda _: VMEM, outs),
        scratch_shapes=list(scratch),
        compiler_params=pltpu.CompilerParams(vmem_limit_bytes=16 * 1024 * 1024),
    )(*args)


def far(x):
    return pltpu.with_memory_space_constraint(x, pltpu.HBM)


def to_each(pieces, axes):
    return lax.all_to_all(pieces, axes, split_axis=0, concat_axis=0, tiled=True)


def ring(x, axis, step):
    count = lax.axis_size(axis)
    return lax.ppermute(x, axis, [(i, (i + step) % count) for i in range(count)])


def beside(faces):
    count = lax.axis_size(SLAB)
    below = lax.ppermute(faces, SLAB, [(i, i + 1) for i in range(count - 1)])
    above = lax.ppermute(faces, SLAB, [(i + 1, i) for i in range(count - 1)])
    return below, above


def swapped(rows):
    half = rows.shape[0] // 2
    return jnp.concatenate([rows[half:], rows[:half]], axis=0)


def flipped(x):
    half = x.shape[1] // 2
    return jnp.concatenate([x[:, half:], x[:, :half]], axis=1)


def pick(index_ref, source_ref, out_ref):
    for j in range(128):
        out_ref[j : j + 1, :] = source_ref[pl.ds(index_ref[0, j], 1), :]


def pack(direction_ref, residual_ref, inverse_ref, lower_ref, upper_ref, out_ref):
    d = direction_ref[...]
    r = residual_ref[...]
    for q in range(4):
        out_ref[q, :, 0:128] = jnp.concatenate([d[:, 64 * q : 64 * q + 64], r[:, 64 * q : 64 * q + 64]], axis=1)
        out_ref[q, :, 128:512] = inverse_ref[...]
        out_ref[q, :, 512:640] = lower_ref[...]
        out_ref[q, :, 640:768] = upper_ref[...]


def make_maps(index_ref, got_ref, factor_ref, maps_ref, faces_ref, all_scr, face_scr):
    factor = mm(got_ref[:, 128:512], got_ref[:, 512:640])
    factor_ref[...] = factor
    all_scr[:, 0:128] = got_ref[:, 0:128]
    all_scr[:, 128:256] = factor
    all_scr[:, 256:384] = got_ref[:, 640:768]
    pick(index_ref, all_scr, face_scr)
    faces_ref[...] = jnp.concatenate([face_scr[0:64, 0:64], face_scr[64:128, 0:64]], axis=1)
    maps_ref[0:128] = -face_scr[:, 128:256]
    maps_ref[128:256] = -face_scr[:, 256:384]


def smooth(index_ref, grp_ref, got_ref, p0, p1, p2, p3, below_ref, above_ref, x_ref, s_ref, faces_ref):
    below = jnp.concatenate([below_ref[:, 0:64], below_ref[:, 64:128]], axis=0)
    above = jnp.concatenate([above_ref[:, 0:64], above_ref[:, 64:128]], axis=0)
    v = jnp.concatenate([got_ref[:, 0:64], below, above], axis=0)
    pieces = (p0, p1, p2, p3)
    image = mm(jnp.concatenate([piece[:, 0:640] for piece in pieces], axis=0), v)
    for step, piece in enumerate(pieces):
        rows = pl.ds(pl.multiple_of(96 * ((grp_ref[0] + 4 - step) % 4), 8), 96)
        x = jnp.concatenate([got_ref[rows, 64:128], image[96 * step : 96 * step + 96]], axis=1)
        x_ref[rows, :] = x
        s_ref[rows, :] = mm(piece[:, 640:736], x)
    pick(index_ref, s_ref, faces_ref)


def solve_slab(
    index_ref, grp_ref, got_ref, p0, p1, p2, p3, factor_ref, x_ref, s_ref, below_ref, above_ref,
    defect_ref, out_ref, solved_scr, face_scr
):
    v = jnp.concatenate([s_ref[...], below_ref[...], above_ref[...]], axis=0)
    pieces = (p0, p1, p2, p3)
    applied = mm(jnp.concatenate([piece[:, 0:640] for piece in pieces], axis=0), v)
    for step in range(4):
        rows = pl.ds(pl.multiple_of(96 * ((grp_ref[0] + 4 - step) % 4), 8), 96)
        defect_ref[rows, :] = x_ref[rows, :] - applied[96 * step : 96 * step + 96]
    x = x_ref[...]
    solved = mm(got_ref[:, 128:512], defect_ref[...])
    solved_scr[...] = solved
    pick(index_ref, solved_scr, face_scr)
    offsets = face_scr[...].T
    turned = x.T
    pulled = -mm(turned, jnp.concatenate([factor_ref[...], got_ref[:, 640:768]], axis=1))
    y = s_ref[...] + solved
    known = jnp.concatenate(
        [
            jnp.sum(x * y, axis=0, keepdims=True),
            jnp.sum(x * flipped(y), axis=0, keepdims=True),
            jnp.sum(got_ref[:, 0:128] * flipped(x), axis=0, keepdims=True),
            jnp.zeros((5, 128), jnp.float32),
        ],
        axis=0,
    )
    for p in range(8):
        for at, part in enumerate((offsets, pulled[:, 0:128], pulled[:, 128:256])):
            out_ref[p, 16 * at : 16 * at + 8] = part[8 * p : 8 * p + 8]
            out_ref[p, 16 * at + 8 : 16 * at + 16] = part[64 + 8 * p : 72 + 8 * p]
        out_ref[p, 48:56] = known


def map_plane(
    x_ref, c_ref, m0, m1, m2, m3, n0, n1, n2, n3, maps_ref, states_f_ref, states_b_ref, plane_ref,
    all_scr, f_scr
):
    for step, (mine, other) in enumerate(((m0, n0), (m1, n1), (m2, n2), (m3, n3))):
        at = 2 * ((x_ref[0] + 4 - step) % 4)
        all_scr[at + c_ref[0]] = mine[...]
        all_scr[at + 1 - c_ref[0]] = other[...]
    for i in range(8):
        keep(maps_ref, i, all_scr[i])
    row = lax.broadcasted_iota(jnp.int32, (128, 128), 0)
    lane = lax.broadcasted_iota(jnp.int32, (128, 128), 1)
    eye = jnp.where(row == lane, 1.0, 0.0).astype(jnp.float32)
    keep(states_f_ref, 0, eye)
    f_scr[0] = all_scr[0, 0:128].T
    for i in range(1, 8):
        keep(states_f_ref, i, f_scr[i - 1])
        f_scr[i] = mm(f_scr[i - 1], kept(maps_ref, i, slice(0, 128)), 1)
    plane_ref[0:128] = f_scr[7]
    keep(states_b_ref, 7, jnp.concatenate([eye, jnp.zeros((128, 128), jnp.float32)], axis=0))
    plane_ref[128:256] = all_scr[7, 128:256].T
    plane_ref[256:384] = f_scr[7]
    for i in reversed(range(7)):
        keep(states_b_ref, i, plane_ref[128:384])
        b = mm(plane_ref[128:384], kept(maps_ref, i, slice(128, 256)), 1)
        plane_ref[128:256] = b[0:128]
        plane_ref[256:384] = b[128:256] + f_scr[i]


def in_lanes(values, place):
    row = lax.broadcasted_iota(jnp.int32, (16, 128), 0)
    lane = lax.broadcasted_iota(jnp.int32, (16, 128), 1)
    target = jnp.where(row < 8, row + 8 * place, row + 56 + 8 * place)
    return jnp.sum(jnp.where(lane == target, values, 0.0), axis=0, keepdims=True)


def sweep_plane(place_ref, got_ref, maps_ref, states_f_ref, states_b_ref, own_f_ref, own_b_ref, out_ref):
    own_f_ref[0] = jnp.zeros((16, 128), jnp.float32)
    own_f_ref[1] = got_ref[0, 0:16]
    for i in range(1, 8):
        f = mm(own_f_ref[i], kept(maps_ref, i, slice(0, 128)), 1) + got_ref[i, 0:16]
        own_f_ref[i + 1] = f
    own_b_ref[7] = jnp.zeros((16, 128), jnp.float32)
    own_b_ref[6] = own_f_ref[8]
    for i in reversed(range(7)):
        b = mm(own_b_ref[i], kept(maps_ref, i, slice(128, 256)), 1) + own_f_ref[i + 1]
        if i > 0:
            own_b_ref[i - 1] = b
    gamma = jnp.zeros((16, 128), jnp.float32)
    delta = gamma
    same = gamma
    cross = gamma
    total = jnp.zeros((8, 128), jnp.float32)
    for i in range(8):
        g = got_ref[i, 16:32]
        h = got_ref[i, 32:48]
        total = total + got_ref[i, 48:56]
        gamma = gamma + mm(g, kept(states_f_ref, i), 1) + mm(h, kept(states_b_ref, i, slice(128, 256)), 1)
        delta = delta + mm(h, kept(states_b_ref, i, slice(0, 128)), 1)
        own_f = own_f_ref[i]
        own_b = own_b_ref[i]
        same = same + g * own_f + h * own_b
        cross = cross + g * swapped(own_f) + h * swapped(own_b)
    place = place_ref[0]
    known = jnp.concatenate(
        [
            total[0:3],
            in_lanes(jnp.sum(same, axis=1, keepdims=True), place),
            in_lanes(jnp.sum(cross, axis=1, keepdims=True), place),
            jnp.zeros((3, 128), jnp.float32),
        ],
        axis=0,
    )
    for z in range(8):
        out_ref[z, 0:16] = own_f_ref[8]
        out_ref[z, 16:32] = b
        out_ref[z, 32:48] = gamma
        out_ref[z, 48:64] = delta
        out_ref[z, 64:72] = known


def solve_planes(
    z_ref, place_ref, sums_ref, a0, a1, a2, a3, a4, b1, b2, b3,
    states_f_ref, states_b_ref, own_f_ref, own_b_ref, out_ref, total_ref, maps_scr, f_scr, b_scr
):
    for step, piece in ((0, a0), (1, a1), (2, a2), (3, a3), (4, a4), (-1, b1), (-2, b2), (-3, b3)):
        maps_scr[(z_ref[0] + 8 - step) % 8] = piece[...]
    f_scr[0] = jnp.zeros((16, 128), jnp.float32)
    f_scr[1] = sums_ref[0, 0:16]
    for z in range(1, 7):
        f_scr[z + 1] = mm(f_scr[z], maps_scr[z, 0:128]) + sums_ref[z, 0:16]
    b_scr[7] = jnp.zeros((16, 128), jnp.float32)
    for z in range(1, 8):
        b_scr[z - 1] = mm(f_scr[z], maps_scr[z, 256:384]) + sums_ref[z, 16:32]
    for z in reversed(range(1, 7)):
        b_scr[z - 1] = b_scr[z - 1] + mm(b_scr[z], maps_scr[z, 128:256])
    same = jnp.zeros((16, 128), jnp.float32)
    cross = same
    known = jnp.zeros((8, 128), jnp.float32)
    for z in range(8):
        gamma = sums_ref[z, 32:48]
        delta = sums_ref[z, 48:64]
        same = same + gamma * f_scr[z] + delta * b_scr[z]
        cross = cross + gamma * swapped(f_scr[z]) + delta * swapped(b_scr[z])
        known = known + sums_ref[z, 64:72]
    total_ref[...] = known
    place = place_ref[0]
    dots = jnp.concatenate(
        [
            known[3:4] + in_lanes(jnp.sum(same, axis=1, keepdims=True), place),
            known[4:5] + in_lanes(jnp.sum(cross, axis=1, keepdims=True), place),
            jnp.zeros((6, 128), jnp.float32),
        ],
        axis=0,
    )
    f = f_scr[z_ref[0]]
    b = b_scr[z_ref[0]]
    for i in range(8):
        out_ref[i, 0:16] = mm(f, kept(states_f_ref, i)) + own_f_ref[i]
        out_ref[i, 16:32] = (
            mm(b, kept(states_b_ref, i, slice(0, 128)))
            + mm(f, kept(states_b_ref, i, slice(128, 256)))
            + own_b_ref[i]
        )
        out_ref[i, 32:40] = dots


def finish(got_ref, back_ref, total_ref, rho_ref, defect_ref, x_ref, s_ref, out_ref):
    def rows(start):
        return jnp.concatenate(
            [back_ref[p, start : start + 8] for p in range(8)]
            + [back_ref[p, start + 8 : start + 16] for p in range(8)],
            axis=0,
        )

    dots = back_ref[0, 32:40]
    for p in range(1, 8):
        dots = dots + back_ref[p, 32:40]
    rest = defect_ref[...] - mm(got_ref[:, 512:640], rows(0), 1)
    precond = s_ref[...] + mm(got_ref[:, 128:512], rest) - mm(got_ref[:, 640:768], rows(16), 1)
    total = total_ref[...]
    step = rho_ref[...] / total[2:3, 0:64]
    same = total[0:1] + dots[0:1]
    cross = total[1:2] + dots[1:2]
    rho = same[:, 0:64] - step * (cross[:, 0:64] + cross[:, 64:128]) + step * (step * same[:, 64:128])
    result = precond[:, 0:64] - step * precond[:, 64:128]
    both = jnp.concatenate([result, x_ref[:, 64:128]], axis=1)
    scales = jnp.broadcast_to(jnp.concatenate([step, rho], axis=1), (8, 128))
    for q in range(4):
        out_ref[q, 0:96] = both[96 * q : 96 * q + 96]
        out_ref[q, 96:104] = scales


def body(
    iterate,
    residual,
    direction,
    prior_rho,
    diag_blocks,
    lower_coupling,
    upper_coupling,
    interface,
    jacobi_inverse,
    slab_inverse,
    lower_factor,
    upper_factor,
):
    def here(axes):
        return lax.axis_index(axes).astype(jnp.int32).reshape(1)

    part = 64
    grp, at_x, at_c, at_z, place = (here(axes) for axes in ("grp", "slab_1", "slab_2", "slab_0", PLANE))
    own_rho = lax.dynamic_slice_in_dim(prior_rho, part * grp[0], part).reshape(1, part)
    grp, at_x, at_c, at_z, place, own_rho, direction, residual = lax.optimization_barrier(
        (grp, at_x, at_c, at_z, place, own_rho, direction, residual)
    )
    operator = jnp.concatenate([diag_blocks, lower_coupling, upper_coupling, jacobi_inverse], axis=1)
    got = to_each(
        call(
            pack,
            shaped(4, 96, 768),
            0,
            *(far(a) for a in (direction, residual, slab_inverse, lower_factor, upper_factor)),
        ),
        "grp",
    ).reshape(384, 768)
    pieces = [operator] + [ring(operator, "grp", step) for step in (1, 2, 3)]
    factor, maps, faces = call(
        make_maps,
        (shaped(384, 128), shaped(256, 128), shaped(64, 128)),
        1,
        interface,
        got,
        scratch=[pltpu.VMEM((384, 384), jnp.float32), pltpu.VMEM((128, 384), jnp.float32)],
    )
    along = [maps] + [ring(maps, "slab_1", step) for step in (1, 2, 3)]
    across = [ring(m, "slab_2", 1) for m in along]
    below, above = beside(faces)
    x, s, faces = call(
        smooth,
        (shaped(384, 128), shaped(384, 128), shaped(128, 128)),
        2,
        interface,
        grp,
        got,
        *pieces,
        below,
        above,
    )
    below, above = beside(faces)
    defect, sent = call(
        solve_slab,
        (shaped(384, 128), shaped(8, 56, 128)),
        2,
        interface,
        grp,
        got,
        *pieces,
        factor,
        x,
        s,
        below,
        above,
        scratch=[pltpu.VMEM((384, 128), jnp.float32), pltpu.VMEM((128, 128), jnp.float32)],
    )
    maps, states_f, states_b, plane = call(
        map_plane,
        (
            shaped(2, 8, 256, 128, dtype=jnp.bfloat16),
            shaped(2, 8, 128, 128, dtype=jnp.bfloat16),
            shaped(2, 8, 256, 128, dtype=jnp.bfloat16),
            shaped(384, 128),
        ),
        2,
        at_x,
        at_c,
        *along,
        *across,
        scratch=[pltpu.VMEM((8, 256, 128), jnp.float32), pltpu.VMEM((8, 128, 128), jnp.float32)],
    )
    ups = [plane]
    for _ in range(1, 5):
        ups.append(ring(ups[-1], "slab_0", 1))
    downs = [plane]
    for _ in range(1, 4):
        downs.append(ring(downs[-1], "slab_0", -1))
    own_f, own_b, sums = call(
        sweep_plane,
        (shaped(9, 16, 128), shaped(8, 16, 128), shaped(8, 72, 128)),
        1,
        place,
        to_each(sent, PLANE),
        far(maps),
        states_f,
        states_b,
    )
    entering, total = call(
        solve_planes,
        (shaped(8, 40, 128), shaped(8, 128)),
        2,
        at_z,
        place,
        to_each(sums, "slab_0"),
        *ups[:4],
        far(ups[4]),
        *downs[1:],
        states_f,
        states_b,
        far(own_f),
        far(own_b),
        scratch=[
            pltpu.VMEM((8, 384, 128), jnp.float32),
            pltpu.VMEM((8, 16, 128), jnp.float32),
            pltpu.VMEM((8, 16, 128), jnp.float32),
        ],
    )
    out = to_each(
        call(
            finish,
            shaped(4, 104, 128),
            0,
            got,
            to_each(entering, PLANE),
            total,
            own_rho,
            defect,
            x,
            s,
        ),
        "grp",
    )
    result = jnp.concatenate([out[q, :96, :part] for q in range(4)], axis=1)
    image = jnp.concatenate([out[q, :96, part:] for q in range(4)], axis=1)
    step_size = jnp.concatenate([out[q, 96, :part] for q in range(4)])
    new_rho = jnp.concatenate([out[q, 96, part:] for q in range(4)])
    new_iterate = iterate + step_size * direction
    new_residual = residual - step_size * image
    new_direction = result + new_rho / prior_rho * direction
    return (new_iterate, new_residual, new_direction, new_rho)


def solution(mesh):
    split = Mesh(
        mesh.devices.reshape(8, 4, 2, mesh.shape["grp"]), ("slab_0", "slab_1", "slab_2", "grp")
    )
    rows = P(SLAB_GRP, None)
    placed = (rows, rows, rows, P(), rows, rows, rows, P(SLAB, None), rows, rows, rows, rows)
    return jax.shard_map(
        body, mesh=split, in_specs=placed, out_specs=(rows, rows, rows, P()), check_vma=False
    )
```

```python
import jax
import jax.numpy as jnp
from jax import lax
from jax.experimental import pallas as pl
from jax.experimental.pallas import tpu as pltpu
from jax.sharding import Mesh
from jax.sharding import PartitionSpec as P

SLAB = ("slab_0", "slab_1", "slab_2")
PLANE = ("slab_1", "slab_2")
SLAB_GRP = ("slab_0", "slab_1", "slab_2", "grp")
VMEM = pl.BlockSpec(memory_space=pltpu.VMEM)
SMEM = pl.BlockSpec(memory_space=pltpu.SMEM)


def halves(x):
    high = x.astype(jnp.bfloat16)
    return high, (x - high.astype(jnp.float32)).astype(jnp.bfloat16)


def mm(left, right, right_dim=0):
    high, low = halves(left)
    right_high, right_low = right if isinstance(right, tuple) else halves(right)

    def dot(a, b):
        return lax.dot_general(
            a, b, (((1,), (right_dim,)), ((), ())), preferred_element_type=jnp.float32
        )

    n = left.shape[0]
    both = dot(jnp.concatenate([high, low], axis=0), right_high)
    return both[:n] + (both[n:] + dot(high, right_low))


def keep(ref, at, x):
    high, low = halves(x)
    ref[0, at] = high
    ref[1, at] = low


def kept(ref, at, rows=slice(None)):
    return ref[0, at, rows], ref[1, at, rows]


def shaped(*shape, dtype=jnp.float32):
    return jax.ShapeDtypeStruct(shape, dtype)


def stored(*shape, dtype=jnp.float32):
    return pltpu.HBM(shape, dtype)


def call(body, outs, smem, *args, scratch=()):
    return pl.pallas_call(
        body,
        out_shape=outs,
        in_specs=[SMEM] * smem + [VMEM] * (len(args) - smem),
        out_specs=jax.tree.map(lambda _: VMEM, outs),
        scratch_shapes=list(scratch),
        compiler_params=pltpu.CompilerParams(vmem_limit_bytes=16 * 1024 * 1024),
    )(*args)


def far(x):
    return pltpu.with_memory_space_constraint(x, pltpu.HBM)


def to_each(pieces, axes):
    return lax.all_to_all(pieces, axes, split_axis=0, concat_axis=0, tiled=True)


def ring(x, axis, step):
    count = lax.axis_size(axis)
    return lax.ppermute(x, axis, [(i, (i + step) % count) for i in range(count)])


def beside(faces):
    count = lax.axis_size(SLAB)
    below = lax.ppermute(faces, SLAB, [(i, i + 1) for i in range(count - 1)])
    above = lax.ppermute(faces, SLAB, [(i + 1, i) for i in range(count - 1)])
    return below, above


def swapped(rows):
    half = rows.shape[0] // 2
    return jnp.concatenate([rows[half:], rows[:half]], axis=0)


def flipped(x):
    half = x.shape[1] // 2
    return jnp.concatenate([x[:, half:], x[:, :half]], axis=1)


def pick(index_ref, source_ref, out_ref):
    for j in range(128):
        out_ref[j : j + 1, :] = source_ref[pl.ds(index_ref[0, j], 1), :]


def pack(direction_ref, residual_ref, inverse_ref, lower_ref, upper_ref, out_ref):
    d = direction_ref[...]
    r = residual_ref[...]
    for q in range(4):
        out_ref[q, :, 0:128] = jnp.concatenate([d[:, 64 * q : 64 * q + 64], r[:, 64 * q : 64 * q + 64]], axis=1)
        out_ref[q, :, 128:512] = inverse_ref[...]
        out_ref[q, :, 512:640] = lower_ref[...]
        out_ref[q, :, 640:768] = upper_ref[...]


def make_maps(index_ref, got_ref, factor_ref, maps_ref, faces_ref, all_scr, face_scr):
    factor = mm(got_ref[:, 128:512], got_ref[:, 512:640])
    factor_ref[...] = factor
    all_scr[:, 0:128] = got_ref[:, 0:128]
    all_scr[:, 128:256] = factor
    all_scr[:, 256:384] = got_ref[:, 640:768]
    pick(index_ref, all_scr, face_scr)
    faces_ref[...] = jnp.concatenate([face_scr[0:64, 0:64], face_scr[64:128, 0:64]], axis=1)
    maps_ref[0:128] = -face_scr[:, 128:256]
    maps_ref[128:256] = -face_scr[:, 256:384]


def smooth(index_ref, grp_ref, got_ref, p0, p1, p2, p3, below_ref, above_ref, x_ref, s_ref, faces_ref):
    below = jnp.concatenate([below_ref[:, 0:64], below_ref[:, 64:128]], axis=0)
    above = jnp.concatenate([above_ref[:, 0:64], above_ref[:, 64:128]], axis=0)
    v = jnp.concatenate([got_ref[:, 0:64], below, above], axis=0)
    pieces = (p0, p1, p2, p3)
    image = mm(jnp.concatenate([piece[:, 0:640] for piece in pieces], axis=0), v)
    for step, piece in enumerate(pieces):
        rows = pl.ds(pl.multiple_of(96 * ((grp_ref[0] + 4 - step) % 4), 8), 96)
        x = jnp.concatenate([got_ref[rows, 64:128], image[96 * step : 96 * step + 96]], axis=1)
        x_ref[rows, :] = x
        s_ref[rows, :] = mm(piece[:, 640:736], x)
    pick(index_ref, s_ref, faces_ref)


def solve_slab(
    index_ref, grp_ref, got_ref, p0, p1, p2, p3, factor_ref, x_ref, s_ref, below_ref, above_ref,
    defect_ref, out_ref, solved_scr, face_scr
):
    v = jnp.concatenate([s_ref[...], below_ref[...], above_ref[...]], axis=0)
    pieces = (p0, p1, p2, p3)
    applied = mm(jnp.concatenate([piece[:, 0:640] for piece in pieces], axis=0), v)
    for step in range(4):
        rows = pl.ds(pl.multiple_of(96 * ((grp_ref[0] + 4 - step) % 4), 8), 96)
        defect_ref[rows, :] = x_ref[rows, :] - applied[96 * step : 96 * step + 96]
    x = x_ref[...]
    solved = mm(got_ref[:, 128:512], defect_ref[...])
    solved_scr[...] = solved
    pick(index_ref, solved_scr, face_scr)
    offsets = face_scr[...].T
    turned = x.T
    pulled = -mm(turned, jnp.concatenate([factor_ref[...], got_ref[:, 640:768]], axis=1))
    y = s_ref[...] + solved
    known = jnp.concatenate(
        [
            jnp.sum(x * y, axis=0, keepdims=True),
            jnp.sum(x * flipped(y), axis=0, keepdims=True),
            jnp.sum(got_ref[:, 0:128] * flipped(x), axis=0, keepdims=True),
            jnp.zeros((5, 128), jnp.float32),
        ],
        axis=0,
    )
    for p in range(8):
        for at, part in enumerate((offsets, pulled[:, 0:128], pulled[:, 128:256])):
            out_ref[p, 16 * at : 16 * at + 8] = part[8 * p : 8 * p + 8]
            out_ref[p, 16 * at + 8 : 16 * at + 16] = part[64 + 8 * p : 72 + 8 * p]
        out_ref[p, 48:56] = known


def map_plane(
    x_ref, c_ref, m0, m1, m2, m3, n0, n1, n2, n3, maps_ref, states_f_ref, states_b_ref, plane_ref,
    all_scr, f_scr
):
    for step, (mine, other) in enumerate(((m0, n0), (m1, n1), (m2, n2), (m3, n3))):
        at = 2 * ((x_ref[0] + 4 - step) % 4)
        all_scr[at + c_ref[0]] = mine[...]
        all_scr[at + 1 - c_ref[0]] = other[...]
    for i in range(8):
        keep(maps_ref, i, all_scr[i])
    row = lax.broadcasted_iota(jnp.int32, (128, 128), 0)
    lane = lax.broadcasted_iota(jnp.int32, (128, 128), 1)
    eye = jnp.where(row == lane, 1.0, 0.0).astype(jnp.float32)
    keep(states_f_ref, 0, eye)
    f_scr[0] = all_scr[0, 0:128].T
    for i in range(1, 8):
        keep(states_f_ref, i, f_scr[i - 1])
        f_scr[i] = mm(f_scr[i - 1], kept(maps_ref, i, slice(0, 128)), 1)
    plane_ref[0:128] = f_scr[7]
    keep(states_b_ref, 7, jnp.concatenate([eye, jnp.zeros((128, 128), jnp.float32)], axis=0))
    plane_ref[128:256] = all_scr[7, 128:256].T
    plane_ref[256:384] = f_scr[7]
    for i in reversed(range(7)):
        keep(states_b_ref, i, plane_ref[128:384])
        b = mm(plane_ref[128:384], kept(maps_ref, i, slice(128, 256)), 1)
        plane_ref[128:256] = b[0:128]
        plane_ref[256:384] = b[128:256] + f_scr[i]


def in_lanes(values, place):
    row = lax.broadcasted_iota(jnp.int32, (16, 128), 0)
    lane = lax.broadcasted_iota(jnp.int32, (16, 128), 1)
    target = jnp.where(row < 8, row + 8 * place, row + 56 + 8 * place)
    return jnp.sum(jnp.where(lane == target, values, 0.0), axis=0, keepdims=True)


def sweep_plane(place_ref, got_ref, maps_ref, states_f_ref, states_b_ref, own_f_ref, own_b_ref, out_ref):
    own_f_ref[0] = jnp.zeros((16, 128), jnp.float32)
    own_f_ref[1] = got_ref[0, 0:16]
    for i in range(1, 8):
        f = mm(own_f_ref[i], kept(maps_ref, i, slice(0, 128)), 1) + got_ref[i, 0:16]
        own_f_ref[i + 1] = f
    own_b_ref[7] = jnp.zeros((16, 128), jnp.float32)
    own_b_ref[6] = own_f_ref[8]
    for i in reversed(range(7)):
        b = mm(own_b_ref[i], kept(maps_ref, i, slice(128, 256)), 1) + own_f_ref[i + 1]
        if i > 0:
            own_b_ref[i - 1] = b
    gamma = jnp.zeros((16, 128), jnp.float32)
    delta = gamma
    same = gamma
    cross = gamma
    total = jnp.zeros((8, 128), jnp.float32)
    for i in range(8):
        g = got_ref[i, 16:32]
        h = got_ref[i, 32:48]
        total = total + got_ref[i, 48:56]
        gamma = gamma + mm(g, kept(states_f_ref, i), 1) + mm(h, kept(states_b_ref, i, slice(128, 256)), 1)
        delta = delta + mm(h, kept(states_b_ref, i, slice(0, 128)), 1)
        own_f = own_f_ref[i]
        own_b = own_b_ref[i]
        same = same + g * own_f + h * own_b
        cross = cross + g * swapped(own_f) + h * swapped(own_b)
    place = place_ref[0]
    known = jnp.concatenate(
        [
            total[0:3],
            in_lanes(jnp.sum(same, axis=1, keepdims=True), place),
            in_lanes(jnp.sum(cross, axis=1, keepdims=True), place),
            jnp.zeros((3, 128), jnp.float32),
        ],
        axis=0,
    )
    for z in range(8):
        out_ref[z, 0:16] = own_f_ref[8]
        out_ref[z, 16:32] = b
        out_ref[z, 32:48] = gamma
        out_ref[z, 48:64] = delta
        out_ref[z, 64:72] = known


def solve_planes(
    z_ref, place_ref, sums_ref, a0, a1, a2, a3, a4, b1, b2, b3,
    states_f_ref, states_b_ref, own_f_ref, own_b_ref, out_ref, total_ref, maps_scr, f_scr, b_scr
):
    for step, piece in ((0, a0), (1, a1), (2, a2), (3, a3), (4, a4), (-1, b1), (-2, b2), (-3, b3)):
        maps_scr[(z_ref[0] + 8 - step) % 8] = piece[...]
    f_scr[0] = jnp.zeros((16, 128), jnp.float32)
    f_scr[1] = sums_ref[0, 0:16]
    for z in range(1, 7):
        f_scr[z + 1] = mm(f_scr[z], maps_scr[z, 0:128]) + sums_ref[z, 0:16]
    b_scr[7] = jnp.zeros((16, 128), jnp.float32)
    for z in range(1, 8):
        b_scr[z - 1] = mm(f_scr[z], maps_scr[z, 256:384]) + sums_ref[z, 16:32]
    for z in reversed(range(1, 7)):
        b_scr[z - 1] = b_scr[z - 1] + mm(b_scr[z], maps_scr[z, 128:256])
    same = jnp.zeros((16, 128), jnp.float32)
    cross = same
    known = jnp.zeros((8, 128), jnp.float32)
    for z in range(8):
        gamma = sums_ref[z, 32:48]
        delta = sums_ref[z, 48:64]
        same = same + gamma * f_scr[z] + delta * b_scr[z]
        cross = cross + gamma * swapped(f_scr[z]) + delta * swapped(b_scr[z])
        known = known + sums_ref[z, 64:72]
    total_ref[...] = known
    place = place_ref[0]
    dots = jnp.concatenate(
        [
            known[3:4] + in_lanes(jnp.sum(same, axis=1, keepdims=True), place),
            known[4:5] + in_lanes(jnp.sum(cross, axis=1, keepdims=True), place),
            jnp.zeros((6, 128), jnp.float32),
        ],
        axis=0,
    )
    f = f_scr[z_ref[0]]
    b = b_scr[z_ref[0]]
    for i in range(8):
        out_ref[i, 0:16] = mm(f, kept(states_f_ref, i)) + own_f_ref[i]
        out_ref[i, 16:32] = (
            mm(b, kept(states_b_ref, i, slice(0, 128)))
            + mm(f, kept(states_b_ref, i, slice(128, 256)))
            + own_b_ref[i]
        )
        out_ref[i, 32:40] = dots


def finish(got_ref, back_ref, total_ref, rho_ref, defect_ref, x_ref, s_ref, out_ref):
    def rows(start):
        return jnp.concatenate(
            [back_ref[p, start : start + 8] for p in range(8)]
            + [back_ref[p, start + 8 : start + 16] for p in range(8)],
            axis=0,
        )

    dots = back_ref[0, 32:40]
    for p in range(1, 8):
        dots = dots + back_ref[p, 32:40]
    rest = defect_ref[...] - mm(got_ref[:, 512:640], rows(0), 1)
    precond = s_ref[...] + mm(got_ref[:, 128:512], rest) - mm(got_ref[:, 640:768], rows(16), 1)
    total = total_ref[...]
    step = rho_ref[...] / total[2:3, 0:64]
    same = total[0:1] + dots[0:1]
    cross = total[1:2] + dots[1:2]
    rho = same[:, 0:64] - step * (cross[:, 0:64] + cross[:, 64:128]) + step * (step * same[:, 64:128])
    result = precond[:, 0:64] - step * precond[:, 64:128]
    both = jnp.concatenate([result, x_ref[:, 64:128]], axis=1)
    scales = jnp.broadcast_to(jnp.concatenate([step, rho], axis=1), (8, 128))
    for q in range(4):
        out_ref[q, 0:96] = both[96 * q : 96 * q + 96]
        out_ref[q, 96:104] = scales


def body(
    iterate,
    residual,
    direction,
    prior_rho,
    diag_blocks,
    lower_coupling,
    upper_coupling,
    interface,
    jacobi_inverse,
    slab_inverse,
    lower_factor,
    upper_factor,
):
    def here(axes):
        return lax.axis_index(axes).astype(jnp.int32).reshape(1)

    part = 64
    grp, at_x, at_c, at_z, place = (here(axes) for axes in ("grp", "slab_1", "slab_2", "slab_0", PLANE))
    own_rho = lax.dynamic_slice_in_dim(prior_rho, part * grp[0], part).reshape(1, part)
    grp, at_x, at_c, at_z, place, own_rho, direction, residual = lax.optimization_barrier(
        (grp, at_x, at_c, at_z, place, own_rho, direction, residual)
    )
    operator = jnp.concatenate([diag_blocks, lower_coupling, upper_coupling, jacobi_inverse], axis=1)
    got = to_each(
        call(
            pack,
            shaped(4, 96, 768),
            0,
            *(far(a) for a in (direction, residual, slab_inverse, lower_factor, upper_factor)),
        ),
        "grp",
    ).reshape(384, 768)
    pieces = [operator] + [ring(operator, "grp", step) for step in (1, 2, 3)]
    factor, maps, faces = call(
        make_maps,
        (shaped(384, 128), shaped(256, 128), shaped(64, 128)),
        1,
        interface,
        got,
        scratch=[pltpu.VMEM((384, 384), jnp.float32), pltpu.VMEM((128, 384), jnp.float32)],
    )
    along = [maps] + [ring(maps, "slab_1", step) for step in (1, 2, 3)]
    across = [ring(m, "slab_2", 1) for m in along]
    below, above = beside(faces)
    x, s, faces = call(
        smooth,
        (shaped(384, 128), shaped(384, 128), shaped(128, 128)),
        2,
        interface,
        grp,
        got,
        *pieces,
        below,
        above,
    )
    below, above = beside(faces)
    defect, sent = call(
        solve_slab,
        (stored(384, 128), stored(8, 56, 128)),
        2,
        interface,
        grp,
        got,
        *pieces,
        factor,
        x,
        s,
        below,
        above,
        scratch=[pltpu.VMEM((384, 128), jnp.float32), pltpu.VMEM((128, 128), jnp.float32)],
    )
    maps, states_f, states_b, plane = call(
        map_plane,
        (
            stored(2, 8, 256, 128, dtype=jnp.bfloat16),
            shaped(2, 8, 128, 128, dtype=jnp.bfloat16),
            shaped(2, 8, 256, 128, dtype=jnp.bfloat16),
            shaped(384, 128),
        ),
        2,
        at_x,
        at_c,
        *map(far, along),
        *map(far, across),
        scratch=[pltpu.VMEM((8, 256, 128), jnp.float32), pltpu.VMEM((8, 128, 128), jnp.float32)],
    )
    ups = [plane]
    for _ in range(1, 5):
        ups.append(ring(ups[-1], "slab_0", 1))
    downs = [plane]
    for _ in range(1, 4):
        downs.append(ring(downs[-1], "slab_0", -1))
    own_f, own_b, sums = call(
        sweep_plane,
        (stored(9, 16, 128), stored(8, 16, 128), stored(8, 72, 128)),
        1,
        place,
        to_each(sent, PLANE),
        far(maps),
        states_f,
        states_b,
    )
    entering, total = call(
        solve_planes,
        (shaped(8, 40, 128), shaped(8, 128)),
        2,
        at_z,
        place,
        to_each(sums, "slab_0"),
        *map(far, ups),
        *map(far, downs[1:]),
        states_f,
        states_b,
        far(own_f),
        far(own_b),
        scratch=[
            pltpu.VMEM((8, 384, 128), jnp.float32),
            pltpu.VMEM((8, 16, 128), jnp.float32),
            pltpu.VMEM((8, 16, 128), jnp.float32),
        ],
    )
    out = to_each(
        call(
            finish,
            shaped(4, 104, 128),
            0,
            got,
            to_each(entering, PLANE),
            total,
            own_rho,
            defect,
            x,
            s,
        ),
        "grp",
    )
    result = jnp.concatenate([out[q, :96, :part] for q in range(4)], axis=1)
    image = jnp.concatenate([out[q, :96, part:] for q in range(4)], axis=1)
    step_size = jnp.concatenate([out[q, 96, :part] for q in range(4)])
    new_rho = jnp.concatenate([out[q, 96, part:] for q in range(4)])
    new_iterate = iterate + step_size * direction
    new_residual = residual - step_size * image
    new_direction = result + new_rho / prior_rho * direction
    return (new_iterate, new_residual, new_direction, new_rho)


def solution(mesh):
    split = Mesh(
        mesh.devices.reshape(8, 4, 2, mesh.shape["grp"]), ("slab_0", "slab_1", "slab_2", "grp")
    )
    rows = P(SLAB_GRP, None)
    placed = (rows, rows, rows, P(), rows, rows, rows, P(SLAB, None), rows, rows, rows, rows)
    return jax.shard_map(
        body, mesh=split, in_specs=placed, out_specs=(rows, rows, rows, P()), check_vma=False
    )
```

```python
import jax
import jax.numpy as jnp
from jax import lax
from jax.experimental import pallas as pl
from jax.experimental.pallas import tpu as pltpu
from jax.sharding import Mesh
from jax.sharding import PartitionSpec as P

SLAB = ("slab_0", "slab_1", "slab_2")
PLANE = ("slab_1", "slab_2")
SLAB_GRP = ("slab_0", "slab_1", "slab_2", "grp")
VMEM = pl.BlockSpec(memory_space=pltpu.VMEM)
SMEM = pl.BlockSpec(memory_space=pltpu.SMEM)


def halves(x):
    high = x.astype(jnp.bfloat16)
    return high, (x - high.astype(jnp.float32)).astype(jnp.bfloat16)


def mm(left, right, right_dim=0):
    high, low = halves(left)
    right_high, right_low = right if isinstance(right, tuple) else halves(right)

    def dot(a, b):
        return lax.dot_general(
            a, b, (((1,), (right_dim,)), ((), ())), preferred_element_type=jnp.float32
        )

    n = left.shape[0]
    both = dot(jnp.concatenate([high, low], axis=0), right_high)
    return both[:n] + (both[n:] + dot(high, right_low))


def keep(ref, at, x):
    high, low = halves(x)
    ref[0, at] = high
    ref[1, at] = low


def kept(ref, at, rows=slice(None)):
    return ref[0, at, rows], ref[1, at, rows]


def shaped(*shape, dtype=jnp.float32):
    return jax.ShapeDtypeStruct(shape, dtype)


def stored(*shape, dtype=jnp.float32):
    return pltpu.HBM(shape, dtype)


def call(body, outs, smem, *args, scratch=()):
    return pl.pallas_call(
        body,
        out_shape=outs,
        in_specs=[SMEM] * smem + [VMEM] * (len(args) - smem),
        out_specs=jax.tree.map(lambda _: VMEM, outs),
        scratch_shapes=list(scratch),
        compiler_params=pltpu.CompilerParams(vmem_limit_bytes=16 * 1024 * 1024),
    )(*args)


def far(x):
    return pltpu.with_memory_space_constraint(x, pltpu.HBM)


def to_each(pieces, axes):
    return lax.all_to_all(pieces, axes, split_axis=0, concat_axis=0, tiled=True)


def ring(x, axis, step):
    count = lax.axis_size(axis)
    return lax.ppermute(x, axis, [(i, (i + step) % count) for i in range(count)])


def beside(faces):
    count = lax.axis_size(SLAB)
    below = lax.ppermute(faces, SLAB, [(i, i + 1) for i in range(count - 1)])
    above = lax.ppermute(faces, SLAB, [(i + 1, i) for i in range(count - 1)])
    return below, above


def swapped(rows):
    half = rows.shape[0] // 2
    return jnp.concatenate([rows[half:], rows[:half]], axis=0)


def flipped(x):
    half = x.shape[1] // 2
    return jnp.concatenate([x[:, half:], x[:, :half]], axis=1)


def pick(index_ref, source_ref, out_ref):
    for j in range(128):
        out_ref[j : j + 1, :] = source_ref[pl.ds(index_ref[0, j], 1), :]


def pack(direction_ref, residual_ref, inverse_ref, lower_ref, upper_ref, out_ref):
    d = direction_ref[...]
    r = residual_ref[...]
    for q in range(4):
        out_ref[q, :, 0:128] = jnp.concatenate([d[:, 64 * q : 64 * q + 64], r[:, 64 * q : 64 * q + 64]], axis=1)
        out_ref[q, :, 128:512] = inverse_ref[...]
        out_ref[q, :, 512:640] = lower_ref[...]
        out_ref[q, :, 640:768] = upper_ref[...]


def make_maps(index_ref, got_ref, factor_ref, maps_ref, faces_ref, all_scr, face_scr):
    factor = mm(got_ref[:, 128:512], got_ref[:, 512:640])
    factor_ref[...] = factor
    all_scr[:, 0:128] = got_ref[:, 0:128]
    all_scr[:, 128:256] = factor
    all_scr[:, 256:384] = got_ref[:, 640:768]
    pick(index_ref, all_scr, face_scr)
    faces_ref[...] = jnp.concatenate([face_scr[0:64, 0:64], face_scr[64:128, 0:64]], axis=1)
    maps_ref[0:128] = -face_scr[:, 128:256]
    maps_ref[128:256] = -face_scr[:, 256:384]


def smooth(index_ref, grp_ref, got_ref, p0, p1, p2, p3, below_ref, above_ref, x_ref, s_ref, faces_ref):
    below = jnp.concatenate([below_ref[:, 0:64], below_ref[:, 64:128]], axis=0)
    above = jnp.concatenate([above_ref[:, 0:64], above_ref[:, 64:128]], axis=0)
    v = jnp.concatenate([got_ref[:, 0:64], below, above], axis=0)
    pieces = (p0, p1, p2, p3)
    image = mm(jnp.concatenate([piece[:, 0:640] for piece in pieces], axis=0), v)
    for step, piece in enumerate(pieces):
        rows = pl.ds(pl.multiple_of(96 * ((grp_ref[0] + 4 - step) % 4), 8), 96)
        x = jnp.concatenate([got_ref[rows, 64:128], image[96 * step : 96 * step + 96]], axis=1)
        x_ref[rows, :] = x
        s_ref[rows, :] = mm(piece[:, 640:736], x)
    pick(index_ref, s_ref, faces_ref)


def solve_slab(
    index_ref, grp_ref, got_ref, p0, p1, p2, p3, factor_ref, x_ref, s_ref, below_ref, above_ref,
    defect_ref, out_ref, solved_scr, face_scr
):
    v = jnp.concatenate([s_ref[...], below_ref[...], above_ref[...]], axis=0)
    pieces = (p0, p1, p2, p3)
    applied = mm(jnp.concatenate([piece[:, 0:640] for piece in pieces], axis=0), v)
    for step in range(4):
        rows = pl.ds(pl.multiple_of(96 * ((grp_ref[0] + 4 - step) % 4), 8), 96)
        defect_ref[rows, :] = x_ref[rows, :] - applied[96 * step : 96 * step + 96]
    x = x_ref[...]
    solved = mm(got_ref[:, 128:512], defect_ref[...])
    solved_scr[...] = solved
    pick(index_ref, solved_scr, face_scr)
    offsets = face_scr[...].T
    turned = x.T
    pulled = -mm(turned, jnp.concatenate([factor_ref[...], got_ref[:, 640:768]], axis=1))
    y = s_ref[...] + solved
    known = jnp.concatenate(
        [
            jnp.sum(x * y, axis=0, keepdims=True),
            jnp.sum(x * flipped(y), axis=0, keepdims=True),
            jnp.sum(got_ref[:, 0:128] * flipped(x), axis=0, keepdims=True),
            jnp.zeros((5, 128), jnp.float32),
        ],
        axis=0,
    )
    for p in range(8):
        for at, part in enumerate((offsets, pulled[:, 0:128], pulled[:, 128:256])):
            out_ref[p, 16 * at : 16 * at + 8] = part[8 * p : 8 * p + 8]
            out_ref[p, 16 * at + 8 : 16 * at + 16] = part[64 + 8 * p : 72 + 8 * p]
        out_ref[p, 48:56] = known


def map_plane(
    x_ref, c_ref, m0, m1, m2, m3, n0, n1, n2, n3, maps_ref, states_f_ref, states_b_ref, half_ref,
    all_scr, f_scr, plane_ref
):
    for step, (mine, other) in enumerate(((m0, n0), (m1, n1), (m2, n2), (m3, n3))):
        at = 2 * ((x_ref[0] + 4 - step) % 4)
        all_scr[at + c_ref[0]] = mine[...]
        all_scr[at + 1 - c_ref[0]] = other[...]
    for i in range(8):
        keep(maps_ref, i, all_scr[i])
    row = lax.broadcasted_iota(jnp.int32, (128, 128), 0)
    lane = lax.broadcasted_iota(jnp.int32, (128, 128), 1)
    eye = jnp.where(row == lane, 1.0, 0.0).astype(jnp.float32)
    keep(states_f_ref, 0, eye)
    f_scr[0] = all_scr[0, 0:128].T
    for i in range(1, 8):
        keep(states_f_ref, i, f_scr[i - 1])
        f_scr[i] = mm(f_scr[i - 1], kept(maps_ref, i, slice(0, 128)), 1)
    plane_ref[0:128] = f_scr[7]
    keep(states_b_ref, 7, jnp.concatenate([eye, jnp.zeros((128, 128), jnp.float32)], axis=0))
    plane_ref[128:256] = all_scr[7, 128:256].T
    plane_ref[256:384] = f_scr[7]
    for i in reversed(range(7)):
        keep(states_b_ref, i, plane_ref[128:384])
        b = mm(plane_ref[128:384], kept(maps_ref, i, slice(128, 256)), 1)
        plane_ref[128:256] = b[0:128]
        plane_ref[256:384] = b[128:256] + f_scr[i]
    for m in range(3):
        own = pl.ds(pl.multiple_of(128 * m + 64 * c_ref[0], 8), 64)
        half_ref[64 * m : 64 * m + 64] = plane_ref[own]


def in_lanes(values, place):
    row = lax.broadcasted_iota(jnp.int32, (16, 128), 0)
    lane = lax.broadcasted_iota(jnp.int32, (16, 128), 1)
    target = jnp.where(row < 8, row + 8 * place, row + 56 + 8 * place)
    return jnp.sum(jnp.where(lane == target, values, 0.0), axis=0, keepdims=True)


def sweep_plane(place_ref, got_ref, maps_ref, states_f_ref, states_b_ref, own_f_ref, own_b_ref, out_ref):
    own_f_ref[0] = jnp.zeros((16, 128), jnp.float32)
    own_f_ref[1] = got_ref[0, 0:16]
    for i in range(1, 8):
        f = mm(own_f_ref[i], kept(maps_ref, i, slice(0, 128)), 1) + got_ref[i, 0:16]
        own_f_ref[i + 1] = f
    own_b_ref[7] = jnp.zeros((16, 128), jnp.float32)
    own_b_ref[6] = own_f_ref[8]
    for i in reversed(range(7)):
        b = mm(own_b_ref[i], kept(maps_ref, i, slice(128, 256)), 1) + own_f_ref[i + 1]
        if i > 0:
            own_b_ref[i - 1] = b
    gamma = jnp.zeros((16, 128), jnp.float32)
    delta = gamma
    same = gamma
    cross = gamma
    total = jnp.zeros((8, 128), jnp.float32)
    for i in range(8):
        g = got_ref[i, 16:32]
        h = got_ref[i, 32:48]
        total = total + got_ref[i, 48:56]
        gamma = gamma + mm(g, kept(states_f_ref, i), 1) + mm(h, kept(states_b_ref, i, slice(128, 256)), 1)
        delta = delta + mm(h, kept(states_b_ref, i, slice(0, 128)), 1)
        own_f = own_f_ref[i]
        own_b = own_b_ref[i]
        same = same + g * own_f + h * own_b
        cross = cross + g * swapped(own_f) + h * swapped(own_b)
    place = place_ref[0]
    known = jnp.concatenate(
        [
            total[0:3],
            in_lanes(jnp.sum(same, axis=1, keepdims=True), place),
            in_lanes(jnp.sum(cross, axis=1, keepdims=True), place),
            jnp.zeros((3, 128), jnp.float32),
        ],
        axis=0,
    )
    for z in range(8):
        out_ref[z, 0:16] = own_f_ref[8]
        out_ref[z, 16:32] = b
        out_ref[z, 32:48] = gamma
        out_ref[z, 48:64] = delta
        out_ref[z, 64:72] = known


def solve_planes(
    c_ref, z_ref, place_ref, sums_ref, p0, p1, p2, p3, p4, p5, p6, p7, q0, q1, q2, q3, q4, q5, q6, q7,
    states_f_ref, states_b_ref, own_f_ref, own_b_ref, out_ref, total_ref, maps_scr, f_scr, b_scr
):
    mine = (p0, p1, p2, p3, p4, p5, p6, p7)
    theirs = (q0, q1, q2, q3, q4, q5, q6, q7)
    for step, own, other in zip((0, 1, -1, 2, -2, 3, -3, 4), mine, theirs):
        z = (z_ref[0] + 8 - step) % 8
        for m in range(3):
            own_rows = pl.ds(pl.multiple_of(128 * m + 64 * c_ref[0], 8), 64)
            other_rows = pl.ds(pl.multiple_of(128 * m + 64 - 64 * c_ref[0], 8), 64)
            maps_scr[z, own_rows] = own[64 * m : 64 * m + 64]
            maps_scr[z, other_rows] = other[64 * m : 64 * m + 64]
    f_scr[0] = jnp.zeros((16, 128), jnp.float32)
    f_scr[1] = sums_ref[0, 0:16]
    for z in range(1, 7):
        f_scr[z + 1] = mm(f_scr[z], maps_scr[z, 0:128]) + sums_ref[z, 0:16]
    b_scr[7] = jnp.zeros((16, 128), jnp.float32)
    for z in range(1, 8):
        b_scr[z - 1] = mm(f_scr[z], maps_scr[z, 256:384]) + sums_ref[z, 16:32]
    for z in reversed(range(1, 7)):
        b_scr[z - 1] = b_scr[z - 1] + mm(b_scr[z], maps_scr[z, 128:256])
    same = jnp.zeros((16, 128), jnp.float32)
    cross = same
    known = jnp.zeros((8, 128), jnp.float32)
    for z in range(8):
        gamma = sums_ref[z, 32:48]
        delta = sums_ref[z, 48:64]
        same = same + gamma * f_scr[z] + delta * b_scr[z]
        cross = cross + gamma * swapped(f_scr[z]) + delta * swapped(b_scr[z])
        known = known + sums_ref[z, 64:72]
    total_ref[...] = known
    place = place_ref[0]
    dots = jnp.concatenate(
        [
            known[3:4] + in_lanes(jnp.sum(same, axis=1, keepdims=True), place),
            known[4:5] + in_lanes(jnp.sum(cross, axis=1, keepdims=True), place),
            jnp.zeros((6, 128), jnp.float32),
        ],
        axis=0,
    )
    f = f_scr[z_ref[0]]
    b = b_scr[z_ref[0]]
    for i in range(8):
        out_ref[i, 0:16] = mm(f, kept(states_f_ref, i)) + own_f_ref[i]
        out_ref[i, 16:32] = (
            mm(b, kept(states_b_ref, i, slice(0, 128)))
            + mm(f, kept(states_b_ref, i, slice(128, 256)))
            + own_b_ref[i]
        )
        out_ref[i, 32:40] = dots


def finish(grp_ref, got_ref, back_ref, total_ref, rho_ref, defect_ref, x_ref, s_ref, out_ref):
    def rows(start):
        return jnp.concatenate(
            [back_ref[p, start : start + 8] for p in range(8)]
            + [back_ref[p, start + 8 : start + 16] for p in range(8)],
            axis=0,
        )

    dots = back_ref[0, 32:40]
    for p in range(1, 8):
        dots = dots + back_ref[p, 32:40]
    rest = defect_ref[...] - mm(got_ref[:, 512:640], rows(0), 1)
    precond = s_ref[...] + mm(got_ref[:, 128:512], rest) - mm(got_ref[:, 640:768], rows(16), 1)
    total = total_ref[...]
    own_rho = rho_ref[:, 0:64]
    for q in range(1, 4):
        own_rho = jnp.where(grp_ref[0] == q, rho_ref[:, 64 * q : 64 * q + 64], own_rho)
    step = own_rho / total[2:3, 0:64]
    same = total[0:1] + dots[0:1]
    cross = total[1:2] + dots[1:2]
    rho = same[:, 0:64] - step * (cross[:, 0:64] + cross[:, 64:128]) + step * (step * same[:, 64:128])
    result = precond[:, 0:64] - step * precond[:, 64:128]
    both = jnp.concatenate([result, x_ref[:, 64:128]], axis=1)
    scales = jnp.broadcast_to(jnp.concatenate([step, rho], axis=1), (8, 128))
    for q in range(4):
        out_ref[q, 0:96] = both[96 * q : 96 * q + 96]
        out_ref[q, 96:104] = scales


def body(
    iterate,
    residual,
    direction,
    prior_rho,
    diag_blocks,
    lower_coupling,
    upper_coupling,
    interface,
    jacobi_inverse,
    slab_inverse,
    lower_factor,
    upper_factor,
):
    def here(axes):
        return lax.axis_index(axes).astype(jnp.int32).reshape(1)

    part = 64
    grp, at_x, at_c, at_z, place = (here(axes) for axes in ("grp", "slab_1", "slab_2", "slab_0", PLANE))
    grp, at_x, at_c, at_z, place, direction, residual = lax.optimization_barrier(
        (grp, at_x, at_c, at_z, place, direction, residual)
    )
    operator = jnp.concatenate([diag_blocks, lower_coupling, upper_coupling, jacobi_inverse], axis=1)
    got = to_each(
        call(
            pack,
            shaped(4, 96, 768),
            0,
            *(far(a) for a in (direction, residual, slab_inverse, lower_factor, upper_factor)),
        ),
        "grp",
    ).reshape(384, 768)
    bulk_up = ring(operator, "grp", 1)
    bulk_down = ring(operator, "grp", 3)
    bulk = [operator, bulk_up, ring(bulk_down, "grp", 3), bulk_down]
    factor, maps, faces = call(
        make_maps,
        (shaped(384, 128), shaped(256, 128), shaped(64, 128)),
        1,
        interface,
        got,
        scratch=[pltpu.VMEM((384, 384), jnp.float32), pltpu.VMEM((128, 384), jnp.float32)],
    )
    along = [maps] + [ring(maps, "slab_1", step) for step in (1, 2, 3)]
    across = [ring(m, "slab_2", 1) for m in along]
    below, above = beside(faces)
    x, s, faces = call(
        smooth,
        (shaped(384, 128), shaped(384, 128), shaped(128, 128)),
        2,
        interface,
        grp,
        got,
        *bulk,
        below,
        above,
    )
    below, above = beside(faces)
    defect, sent = call(
        solve_slab,
        (stored(384, 128), stored(8, 56, 128)),
        2,
        interface,
        grp,
        got,
        *bulk,
        factor,
        x,
        s,
        below,
        above,
        scratch=[pltpu.VMEM((384, 128), jnp.float32), pltpu.VMEM((128, 128), jnp.float32)],
    )
    maps, states_f, states_b, half = call(
        map_plane,
        (
            stored(2, 8, 256, 128, dtype=jnp.bfloat16),
            shaped(2, 8, 128, 128, dtype=jnp.bfloat16),
            shaped(2, 8, 256, 128, dtype=jnp.bfloat16),
            shaped(192, 128),
        ),
        2,
        at_x,
        at_c,
        *along,
        *across,
        scratch=[
            pltpu.VMEM((8, 256, 128), jnp.float32),
            pltpu.VMEM((8, 128, 128), jnp.float32),
            pltpu.VMEM((384, 128), jnp.float32),
        ],
    )
    ups = [half]
    for _ in range(1, 5):
        ups.append(ring(ups[-1], "slab_0", 1))
    downs = [half]
    for _ in range(1, 4):
        downs.append(ring(downs[-1], "slab_0", -1))
    pieces = [half, ups[1], downs[1], ups[2], downs[2], ups[3], downs[3], ups[4]]
    others = [ring(piece, "slab_2", 1) for piece in pieces]
    own_f, own_b, sums = call(
        sweep_plane,
        (stored(9, 16, 128), stored(8, 16, 128), stored(8, 72, 128)),
        1,
        place,
        to_each(sent, PLANE),
        far(maps),
        states_f,
        states_b,
    )
    entering, total = call(
        solve_planes,
        (shaped(8, 40, 128), shaped(8, 128)),
        3,
        at_c,
        at_z,
        place,
        to_each(sums, "slab_0"),
        *map(far, pieces),
        *map(far, others),
        states_f,
        states_b,
        far(own_f),
        far(own_b),
        scratch=[
            pltpu.VMEM((8, 384, 128), jnp.float32),
            pltpu.VMEM((8, 16, 128), jnp.float32),
            pltpu.VMEM((8, 16, 128), jnp.float32),
        ],
    )
    out = to_each(
        call(
            finish,
            shaped(4, 104, 128),
            1,
            grp,
            got,
            to_each(entering, PLANE),
            total,
            prior_rho.reshape(1, 4 * part),
            defect,
            x,
            s,
        ),
        "grp",
    )
    result = jnp.concatenate([out[q, :96, :part] for q in range(4)], axis=1)
    image = jnp.concatenate([out[q, :96, part:] for q in range(4)], axis=1)
    step_size = jnp.concatenate([out[q, 96, :part] for q in range(4)])
    new_rho = jnp.concatenate([out[q, 96, part:] for q in range(4)])
    new_iterate = iterate + step_size * direction
    new_residual = residual - step_size * image
    new_direction = result + new_rho / prior_rho * direction
    return (new_iterate, new_residual, new_direction, new_rho)


def solution(mesh):
    split = Mesh(
        mesh.devices.reshape(8, 4, 2, mesh.shape["grp"]), ("slab_0", "slab_1", "slab_2", "grp")
    )
    rows = P(SLAB_GRP, None)
    placed = (rows, rows, rows, P(), rows, rows, rows, P(SLAB, None), rows, rows, rows, rows)
    return jax.shard_map(
        body, mesh=split, in_specs=placed, out_specs=(rows, rows, rows, P()), check_vma=False
    )
```

```python
import jax
import jax.numpy as jnp
from jax import lax
from jax.experimental import pallas as pl
from jax.experimental.pallas import tpu as pltpu
from jax.sharding import Mesh
from jax.sharding import PartitionSpec as P

SLAB = ("slab_0", "slab_1", "slab_2")
PLANE = ("slab_1", "slab_2")
SLAB_GRP = ("slab_0", "slab_1", "slab_2", "grp")
VMEM = pl.BlockSpec(memory_space=pltpu.VMEM)
SMEM = pl.BlockSpec(memory_space=pltpu.SMEM)


def halves(x):
    high = x.astype(jnp.bfloat16)
    return high, (x - high.astype(jnp.float32)).astype(jnp.bfloat16)


def mm(left, right, right_dim=0):
    high, low = halves(left)
    right_high, right_low = right if isinstance(right, tuple) else halves(right)

    def dot(a, b):
        return lax.dot_general(
            a, b, (((1,), (right_dim,)), ((), ())), preferred_element_type=jnp.float32
        )

    n = left.shape[0]
    both = dot(jnp.concatenate([high, low], axis=0), right_high)
    return both[:n] + (both[n:] + dot(high, right_low))


def keep(ref, at, x):
    high, low = halves(x)
    ref[0, at] = high
    ref[1, at] = low


def kept(ref, at, rows=slice(None)):
    return ref[0, at, rows], ref[1, at, rows]


def shaped(*shape, dtype=jnp.float32):
    return jax.ShapeDtypeStruct(shape, dtype)


def stored(*shape, dtype=jnp.float32):
    return pltpu.HBM(shape, dtype)


def call(body, outs, smem, *args, scratch=()):
    return pl.pallas_call(
        body,
        out_shape=outs,
        in_specs=[SMEM] * smem + [VMEM] * (len(args) - smem),
        out_specs=jax.tree.map(lambda _: VMEM, outs),
        scratch_shapes=list(scratch),
        compiler_params=pltpu.CompilerParams(vmem_limit_bytes=16 * 1024 * 1024),
    )(*args)


def far(x):
    return pltpu.with_memory_space_constraint(x, pltpu.HBM)


def to_each(pieces, axes):
    return lax.all_to_all(pieces, axes, split_axis=0, concat_axis=0, tiled=True)


def ring(x, axis, step):
    count = lax.axis_size(axis)
    return lax.ppermute(x, axis, [(i, (i + step) % count) for i in range(count)])


def beside(faces):
    count = lax.axis_size(SLAB)
    below = lax.ppermute(faces, SLAB, [(i, i + 1) for i in range(count - 1)])
    above = lax.ppermute(faces, SLAB, [(i + 1, i) for i in range(count - 1)])
    return below, above


def swapped(rows):
    half = rows.shape[0] // 2
    return jnp.concatenate([rows[half:], rows[:half]], axis=0)


def flipped(x):
    half = x.shape[1] // 2
    return jnp.concatenate([x[:, half:], x[:, :half]], axis=1)


def pick(index_ref, source_ref, out_ref):
    for j in range(128):
        out_ref[j : j + 1, :] = source_ref[pl.ds(index_ref[0, j], 1), :]


def pack(direction_ref, residual_ref, inverse_ref, lower_ref, upper_ref, out_ref, coarse_ref):
    coarse_ref[:, 0:384] = inverse_ref[...]
    coarse_ref[:, 384:512] = lower_ref[...]
    coarse_ref[:, 512:640] = upper_ref[...]
    d = direction_ref[...]
    r = residual_ref[...]
    for q in range(4):
        out_ref[q] = jnp.concatenate([d[:, 64 * q : 64 * q + 64], r[:, 64 * q : 64 * q + 64]], axis=1)


def make_maps(
    index_ref, grp_ref, fields_ref, c0, c1, c2, c3, got_ref, factor_ref, maps_ref, faces_ref, all_scr, face_scr
):
    for step, piece in enumerate((c0, c1, c2, c3)):
        rows = pl.ds(pl.multiple_of(96 * ((grp_ref[0] + 4 - step) % 4), 8), 96)
        got_ref[rows, 128:768] = piece[...]
    got_ref[:, 0:128] = fields_ref[...]
    factor = mm(got_ref[:, 128:512], got_ref[:, 512:640])
    factor_ref[...] = factor
    all_scr[:, 0:128] = got_ref[:, 0:128]
    all_scr[:, 128:256] = factor
    all_scr[:, 256:384] = got_ref[:, 640:768]
    pick(index_ref, all_scr, face_scr)
    faces_ref[...] = jnp.concatenate([face_scr[0:64, 0:64], face_scr[64:128, 0:64]], axis=1)
    maps_ref[0:128] = -face_scr[:, 128:256]
    maps_ref[128:256] = -face_scr[:, 256:384]


def smooth(index_ref, grp_ref, got_ref, p0, p1, p2, p3, below_ref, above_ref, x_ref, s_ref, faces_ref):
    below = jnp.concatenate([below_ref[:, 0:64], below_ref[:, 64:128]], axis=0)
    above = jnp.concatenate([above_ref[:, 0:64], above_ref[:, 64:128]], axis=0)
    v = jnp.concatenate([got_ref[:, 0:64], below, above], axis=0)
    pieces = (p0, p1, p2, p3)
    image = mm(jnp.concatenate([piece[:, 0:640] for piece in pieces], axis=0), v)
    for step, piece in enumerate(pieces):
        rows = pl.ds(pl.multiple_of(96 * ((grp_ref[0] + 4 - step) % 4), 8), 96)
        x = jnp.concatenate([got_ref[rows, 64:128], image[96 * step : 96 * step + 96]], axis=1)
        x_ref[rows, :] = x
        s_ref[rows, :] = mm(piece[:, 640:736], x)
    pick(index_ref, s_ref, faces_ref)


def solve_slab(
    index_ref, grp_ref, got_ref, p0, p1, p2, p3, factor_ref, x_ref, s_ref, below_ref, above_ref,
    defect_ref, out_ref, solved_scr, face_scr
):
    v = jnp.concatenate([s_ref[...], below_ref[...], above_ref[...]], axis=0)
    pieces = (p0, p1, p2, p3)
    applied = mm(jnp.concatenate([piece[:, 0:640] for piece in pieces], axis=0), v)
    for step in range(4):
        rows = pl.ds(pl.multiple_of(96 * ((grp_ref[0] + 4 - step) % 4), 8), 96)
        defect_ref[rows, :] = x_ref[rows, :] - applied[96 * step : 96 * step + 96]
    x = x_ref[...]
    solved = mm(got_ref[:, 128:512], defect_ref[...])
    solved_scr[...] = solved
    pick(index_ref, solved_scr, face_scr)
    offsets = face_scr[...].T
    turned = x.T
    pulled = -mm(turned, jnp.concatenate([factor_ref[...], got_ref[:, 640:768]], axis=1))
    y = s_ref[...] + solved
    known = jnp.concatenate(
        [
            jnp.sum(x * y, axis=0, keepdims=True),
            jnp.sum(x * flipped(y), axis=0, keepdims=True),
            jnp.sum(got_ref[:, 0:128] * flipped(x), axis=0, keepdims=True),
            jnp.zeros((5, 128), jnp.float32),
        ],
        axis=0,
    )
    for p in range(8):
        for at, part in enumerate((offsets, pulled[:, 0:128], pulled[:, 128:256])):
            out_ref[p, 16 * at : 16 * at + 8] = part[8 * p : 8 * p + 8]
            out_ref[p, 16 * at + 8 : 16 * at + 16] = part[64 + 8 * p : 72 + 8 * p]
        out_ref[p, 48:56] = known


def map_plane(
    x_ref, c_ref, m0, m1, m2, m3, n0, n1, n2, n3, maps_ref, states_f_ref, states_b_ref, half_ref,
    all_scr, f_scr, plane_ref
):
    for step, (mine, other) in enumerate(((m0, n0), (m1, n1), (m2, n2), (m3, n3))):
        at = 2 * ((x_ref[0] + 4 - step) % 4)
        all_scr[at + c_ref[0]] = mine[...]
        all_scr[at + 1 - c_ref[0]] = other[...]
    for i in range(8):
        keep(maps_ref, i, all_scr[i])
    row = lax.broadcasted_iota(jnp.int32, (128, 128), 0)
    lane = lax.broadcasted_iota(jnp.int32, (128, 128), 1)
    eye = jnp.where(row == lane, 1.0, 0.0).astype(jnp.float32)
    keep(states_f_ref, 0, eye)
    f_scr[0] = all_scr[0, 0:128].T
    for i in range(1, 8):
        keep(states_f_ref, i, f_scr[i - 1])
        f_scr[i] = mm(f_scr[i - 1], kept(maps_ref, i, slice(0, 128)), 1)
    plane_ref[0:128] = f_scr[7]
    keep(states_b_ref, 7, jnp.concatenate([eye, jnp.zeros((128, 128), jnp.float32)], axis=0))
    plane_ref[128:256] = all_scr[7, 128:256].T
    plane_ref[256:384] = f_scr[7]
    for i in reversed(range(7)):
        keep(states_b_ref, i, plane_ref[128:384])
        b = mm(plane_ref[128:384], kept(maps_ref, i, slice(128, 256)), 1)
        plane_ref[128:256] = b[0:128]
        plane_ref[256:384] = b[128:256] + f_scr[i]
    for m in range(3):
        own = pl.ds(pl.multiple_of(128 * m + 64 * c_ref[0], 8), 64)
        half_ref[64 * m : 64 * m + 64] = plane_ref[own]


def in_lanes(values, place):
    row = lax.broadcasted_iota(jnp.int32, (16, 128), 0)
    lane = lax.broadcasted_iota(jnp.int32, (16, 128), 1)
    target = jnp.where(row < 8, row + 8 * place, row + 56 + 8 * place)
    return jnp.sum(jnp.where(lane == target, values, 0.0), axis=0, keepdims=True)


def sweep_plane(place_ref, got_ref, maps_ref, states_f_ref, states_b_ref, own_f_ref, own_b_ref, out_ref):
    own_f_ref[0] = jnp.zeros((16, 128), jnp.float32)
    own_f_ref[1] = got_ref[0, 0:16]
    for i in range(1, 8):
        f = mm(own_f_ref[i], kept(maps_ref, i, slice(0, 128)), 1) + got_ref[i, 0:16]
        own_f_ref[i + 1] = f
    own_b_ref[7] = jnp.zeros((16, 128), jnp.float32)
    own_b_ref[6] = own_f_ref[8]
    for i in reversed(range(7)):
        b = mm(own_b_ref[i], kept(maps_ref, i, slice(128, 256)), 1) + own_f_ref[i + 1]
        if i > 0:
            own_b_ref[i - 1] = b
    gamma = jnp.zeros((16, 128), jnp.float32)
    delta = gamma
    same = gamma
    cross = gamma
    total = jnp.zeros((8, 128), jnp.float32)
    for i in range(8):
        g = got_ref[i, 16:32]
        h = got_ref[i, 32:48]
        total = total + got_ref[i, 48:56]
        gamma = gamma + mm(g, kept(states_f_ref, i), 1) + mm(h, kept(states_b_ref, i, slice(128, 256)), 1)
        delta = delta + mm(h, kept(states_b_ref, i, slice(0, 128)), 1)
        own_f = own_f_ref[i]
        own_b = own_b_ref[i]
        same = same + g * own_f + h * own_b
        cross = cross + g * swapped(own_f) + h * swapped(own_b)
    place = place_ref[0]
    known = jnp.concatenate(
        [
            total[0:3],
            in_lanes(jnp.sum(same, axis=1, keepdims=True), place),
            in_lanes(jnp.sum(cross, axis=1, keepdims=True), place),
            jnp.zeros((3, 128), jnp.float32),
        ],
        axis=0,
    )
    for z in range(8):
        out_ref[z, 0:16] = own_f_ref[8]
        out_ref[z, 16:32] = b
        out_ref[z, 32:48] = gamma
        out_ref[z, 48:64] = delta
        out_ref[z, 64:72] = known


def solve_planes(
    c_ref, z_ref, place_ref, sums_ref, p0, p1, p2, p3, p4, p5, p6, p7, q0, q1, q2, q3, q4, q5, q6, q7,
    states_f_ref, states_b_ref, own_f_ref, own_b_ref, out_ref, total_ref, maps_scr, f_scr, b_scr
):
    mine = (p0, p1, p2, p3, p4, p5, p6, p7)
    theirs = (q0, q1, q2, q3, q4, q5, q6, q7)
    for step, own, other in zip((0, 1, -1, 2, -2, 3, -3, 4), mine, theirs):
        z = (z_ref[0] + 8 - step) % 8
        for m in range(3):
            own_rows = pl.ds(pl.multiple_of(128 * m + 64 * c_ref[0], 8), 64)
            other_rows = pl.ds(pl.multiple_of(128 * m + 64 - 64 * c_ref[0], 8), 64)
            maps_scr[z, own_rows] = own[64 * m : 64 * m + 64]
            maps_scr[z, other_rows] = other[64 * m : 64 * m + 64]
    f_scr[0] = jnp.zeros((16, 128), jnp.float32)
    f_scr[1] = sums_ref[0, 0:16]
    for z in range(1, 7):
        f_scr[z + 1] = mm(f_scr[z], maps_scr[z, 0:128]) + sums_ref[z, 0:16]
    b_scr[7] = jnp.zeros((16, 128), jnp.float32)
    for z in range(1, 8):
        b_scr[z - 1] = mm(f_scr[z], maps_scr[z, 256:384]) + sums_ref[z, 16:32]
    for z in reversed(range(1, 7)):
        b_scr[z - 1] = b_scr[z - 1] + mm(b_scr[z], maps_scr[z, 128:256])
    same = jnp.zeros((16, 128), jnp.float32)
    cross = same
    known = jnp.zeros((8, 128), jnp.float32)
    for z in range(8):
        gamma = sums_ref[z, 32:48]
        delta = sums_ref[z, 48:64]
        same = same + gamma * f_scr[z] + delta * b_scr[z]
        cross = cross + gamma * swapped(f_scr[z]) + delta * swapped(b_scr[z])
        known = known + sums_ref[z, 64:72]
    total_ref[...] = known
    place = place_ref[0]
    dots = jnp.concatenate(
        [
            known[3:4] + in_lanes(jnp.sum(same, axis=1, keepdims=True), place),
            known[4:5] + in_lanes(jnp.sum(cross, axis=1, keepdims=True), place),
            jnp.zeros((6, 128), jnp.float32),
        ],
        axis=0,
    )
    f = f_scr[z_ref[0]]
    b = b_scr[z_ref[0]]
    for i in range(8):
        out_ref[i, 0:16] = mm(f, kept(states_f_ref, i)) + own_f_ref[i]
        out_ref[i, 16:32] = (
            mm(b, kept(states_b_ref, i, slice(0, 128)))
            + mm(f, kept(states_b_ref, i, slice(128, 256)))
            + own_b_ref[i]
        )
        out_ref[i, 32:40] = dots


def finish(grp_ref, got_ref, back_ref, total_ref, rho_ref, defect_ref, x_ref, s_ref, out_ref):
    def rows(start):
        return jnp.concatenate(
            [back_ref[p, start : start + 8] for p in range(8)]
            + [back_ref[p, start + 8 : start + 16] for p in range(8)],
            axis=0,
        )

    dots = back_ref[0, 32:40]
    for p in range(1, 8):
        dots = dots + back_ref[p, 32:40]
    rest = defect_ref[...] - mm(got_ref[:, 512:640], rows(0), 1)
    precond = s_ref[...] + mm(got_ref[:, 128:512], rest) - mm(got_ref[:, 640:768], rows(16), 1)
    total = total_ref[...]
    own_rho = rho_ref[:, 0:64]
    for q in range(1, 4):
        own_rho = jnp.where(grp_ref[0] == q, rho_ref[:, 64 * q : 64 * q + 64], own_rho)
    step = own_rho / total[2:3, 0:64]
    same = total[0:1] + dots[0:1]
    cross = total[1:2] + dots[1:2]
    rho = same[:, 0:64] - step * (cross[:, 0:64] + cross[:, 64:128]) + step * (step * same[:, 64:128])
    result = precond[:, 0:64] - step * precond[:, 64:128]
    both = jnp.concatenate([result, x_ref[:, 64:128]], axis=1)
    scales = jnp.broadcast_to(jnp.concatenate([step, rho], axis=1), (8, 128))
    for q in range(4):
        out_ref[q, 0:96] = both[96 * q : 96 * q + 96]
        out_ref[q, 96:104] = scales


def body(
    iterate,
    residual,
    direction,
    prior_rho,
    diag_blocks,
    lower_coupling,
    upper_coupling,
    interface,
    jacobi_inverse,
    slab_inverse,
    lower_factor,
    upper_factor,
):
    def here(axes):
        return lax.axis_index(axes).astype(jnp.int32).reshape(1)

    part = 64
    grp, at_x, at_c, at_z, place = (here(axes) for axes in ("grp", "slab_1", "slab_2", "slab_0", PLANE))
    grp, at_x, at_c, at_z, place, direction, residual = lax.optimization_barrier(
        (grp, at_x, at_c, at_z, place, direction, residual)
    )
    operator = jnp.concatenate([diag_blocks, lower_coupling, upper_coupling, jacobi_inverse], axis=1)
    sent, coarse = call(
        pack,
        (shaped(4, 96, 128), shaped(96, 640)),
        0,
        *(far(a) for a in (direction, residual, slab_inverse, lower_factor, upper_factor)),
    )
    fields = to_each(sent, "grp").reshape(384, 128)
    coarse_up = ring(coarse, "grp", 1)
    coarse_down = ring(coarse, "grp", 3)
    coarse = [coarse, coarse_up, ring(coarse_up, "grp", 1), coarse_down]
    bulk_up = ring(operator, "grp", 1)
    bulk_down = ring(operator, "grp", 3)
    bulk = [operator, bulk_up, ring(bulk_down, "grp", 3), bulk_down]
    got, factor, maps, faces = call(
        make_maps,
        (shaped(384, 768), shaped(384, 128), shaped(256, 128), shaped(64, 128)),
        2,
        interface,
        grp,
        fields,
        far(coarse[0]),
        *coarse[1:],
        scratch=[pltpu.VMEM((384, 384), jnp.float32), pltpu.VMEM((128, 384), jnp.float32)],
    )
    along = [maps] + [ring(maps, "slab_1", step) for step in (1, 2, 3)]
    across = [ring(m, "slab_2", 1) for m in along]
    below, above = beside(faces)
    x, s, faces = call(
        smooth,
        (shaped(384, 128), shaped(384, 128), shaped(128, 128)),
        2,
        interface,
        grp,
        got,
        *bulk,
        below,
        above,
    )
    below, above = beside(faces)
    defect, sent = call(
        solve_slab,
        (stored(384, 128), stored(8, 56, 128)),
        2,
        interface,
        grp,
        got,
        *bulk,
        factor,
        x,
        s,
        below,
        above,
        scratch=[pltpu.VMEM((384, 128), jnp.float32), pltpu.VMEM((128, 128), jnp.float32)],
    )
    maps, states_f, states_b, half = call(
        map_plane,
        (
            stored(2, 8, 256, 128, dtype=jnp.bfloat16),
            shaped(2, 8, 128, 128, dtype=jnp.bfloat16),
            shaped(2, 8, 256, 128, dtype=jnp.bfloat16),
            shaped(192, 128),
        ),
        2,
        at_x,
        at_c,
        *along,
        *across,
        scratch=[
            pltpu.VMEM((8, 256, 128), jnp.float32),
            pltpu.VMEM((8, 128, 128), jnp.float32),
            pltpu.VMEM((384, 128), jnp.float32),
        ],
    )
    ups = [half]
    for _ in range(1, 5):
        ups.append(ring(ups[-1], "slab_0", 1))
    downs = [half]
    for _ in range(1, 4):
        downs.append(ring(downs[-1], "slab_0", -1))
    pieces = [half, ups[1], downs[1], ups[2], downs[2], ups[3], downs[3], ups[4]]
    others = [ring(piece, "slab_2", 1) for piece in pieces]
    own_f, own_b, sums = call(
        sweep_plane,
        (stored(9, 16, 128), stored(8, 16, 128), stored(8, 72, 128)),
        1,
        place,
        to_each(sent, PLANE),
        far(maps),
        states_f,
        states_b,
    )
    entering, total = call(
        solve_planes,
        (shaped(8, 40, 128), shaped(8, 128)),
        3,
        at_c,
        at_z,
        place,
        to_each(sums, "slab_0"),
        *map(far, pieces),
        *map(far, others),
        states_f,
        states_b,
        far(own_f),
        far(own_b),
        scratch=[
            pltpu.VMEM((8, 384, 128), jnp.float32),
            pltpu.VMEM((8, 16, 128), jnp.float32),
            pltpu.VMEM((8, 16, 128), jnp.float32),
        ],
    )
    out = to_each(
        call(
            finish,
            shaped(4, 104, 128),
            1,
            grp,
            got,
            to_each(entering, PLANE),
            total,
            prior_rho.reshape(1, 4 * part),
            defect,
            x,
            s,
        ),
        "grp",
    )
    result = jnp.concatenate([out[q, :96, :part] for q in range(4)], axis=1)
    image = jnp.concatenate([out[q, :96, part:] for q in range(4)], axis=1)
    step_size = jnp.concatenate([out[q, 96, :part] for q in range(4)])
    new_rho = jnp.concatenate([out[q, 96, part:] for q in range(4)])
    new_iterate = iterate + step_size * direction
    new_residual = residual - step_size * image
    new_direction = result + new_rho / prior_rho * direction
    return (new_iterate, new_residual, new_direction, new_rho)


def solution(mesh):
    split = Mesh(
        mesh.devices.reshape(8, 4, 2, mesh.shape["grp"]), ("slab_0", "slab_1", "slab_2", "grp")
    )
    rows = P(SLAB_GRP, None)
    placed = (rows, rows, rows, P(), rows, rows, rows, P(SLAB, None), rows, rows, rows, rows)
    return jax.shard_map(
        body, mesh=split, in_specs=placed, out_specs=(rows, rows, rows, P()), check_vma=False
    )
```
